32 devices in a mesh: seq: 8 (over z, x), head: 4 (over y, core).
Axes of the slice: x: 2, y: 2, z: 4, core: 2. Of those that a mesh axis runs over, the one named last changes fastest.
Arguments:
- patches: bfloat16 [32768, 768], P('seq'), may hold values from -6 to 6
- slot_image: int32 [128], P('seq'), may hold values from -1 to 63, as said below
- slot_dest: int32 [128], P('seq'), may hold values from -1 to 63, as said below
- enc_gain: float32 [768], replicated, may hold values from 0.1 to 1.9
- w_qkv: bfloat16 [3, 768, 768], P(None, None, 'head'), may hold values from -1.2 to 1.2
- w_out: bfloat16 [768, 768], P('head'), may hold values from -0.21875 to 0.21875
- fast_gain: float32 [768], replicated, may hold values from 0.1 to 1.9
- w_fast: bfloat16 [3, 768, 768], P(None, None, 'head'), may hold values from -0.21875 to 0.21875
- w_rate: bfloat16 [768, 4], P(None, 'head'), may hold values from -0.21875 to 0.21875
- fast_gate_up: float32 [4, 2, 192, 384], P('head'), may hold values from -0.4375 to 0.4375
- fast_down: float32 [4, 384, 192], P('head'), may hold values from -0.3125 to 0.3125
Outputs:
- view_out: bfloat16 [16384, 768], P('seq', 'head')
The draws below stay inside these ranges and needn't reach their ends.
Inputs may be any that keep to these rules, and one draw needn't show every extreme that they name: slot_dest gives for each slot the view-order block that its block becomes, or -1 for an empty slot; every view-order block is named by exactly one slot. Slots 2i and 2i + 1 of one seq index are both empty or name view blocks 2m and 2m + 1. The slots of one seq index name at most 2 blocks of any one view shard (blocks s * 8 to (s + 1) * 8 - 1), and some seq index uses all of its slots. slot_image is -1 exactly where slot_dest is -1; an image is one block or the two blocks of a slot pair, and different images have different ids.
All inputs are finite; a program needn't handle non-finite values.
Results may differ from the reference program's by a relative error of at most 0.035.
Values may be sent and summed in bfloat16 or wider, within the bound.
A program may use at most 128 MiB of HBM per device.

```python
import math
import jax
import jax.numpy as jnp
from jax import lax

D = 768
HDIM = 64
FHEADS = 4
FW = 192
FH = 384
BLK = 256
BLK_DEV = 8
WSLOT = 16
VTOKENS = 16384
WTOKENS = 32768
N_SEQ = 8


def source_rank(source, busiest):
    half_away = (busiest + N_SEQ // 2) % N_SEQ
    next_one = (busiest + 1) % N_SEQ
    rotated = (source - busiest - 2) % N_SEQ
    rest = jnp.where(rotated < N_SEQ // 2 - 2, rotated + 2, rotated + 1)
    return jnp.where(source == half_away, 0, jnp.where(source == next_one, 1, rest))


def slot_layout(key):
    key_parts = jax.random.split(jax.random.fold_in(key, 41), 5)
    bins_dev = BLK_DEV // 2
    busiest = jax.random.randint(key_parts[0], (), 0, N_SEQ)
    shifts = jax.random.permutation(key_parts[2], N_SEQ - 1)
    paired = jax.random.randint(key_parts[3], (N_SEQ, bins_dev), 0, 2)
    places = jax.vmap(lambda part_key: jax.random.permutation(part_key, BLK_DEV))(jax.random.split(key_parts[4], N_SEQ))
    source = jnp.broadcast_to(jnp.arange(N_SEQ, dtype=jnp.int32)[:, None], (N_SEQ, bins_dev))
    column = jnp.broadcast_to(jnp.arange(bins_dev, dtype=jnp.int32)[None, :], (N_SEQ, bins_dev))
    ordinal = column * N_SEQ + source_rank(source, busiest)
    to_busiest = ordinal < BLK_DEV
    offset_bin = shifts[column % (N_SEQ - 1)]
    spread_to = (busiest + 1 + (source + offset_bin) % (N_SEQ - 1)) % N_SEQ
    worker = jnp.where(to_busiest, busiest, spread_to)
    place_bin = jnp.where(to_busiest, ordinal, 2 * column + (source == N_SEQ - 1).astype(jnp.int32))
    place_bin = places[worker, place_bin]
    view_first = source * BLK_DEV + 2 * column
    slot_first = worker * (2 * BLK_DEV) + 2 * place_bin
    second_image = jnp.where(paired == 1, view_first, view_first + 1)
    slot_all = jnp.concatenate([slot_first.reshape(-1), slot_first.reshape(-1) + 1]).astype(jnp.int32)
    view_all = jnp.concatenate([view_first.reshape(-1), view_first.reshape(-1) + 1]).astype(jnp.int32)
    image_all = jnp.concatenate([view_first.reshape(-1), second_image.reshape(-1)]).astype(jnp.int32)
    unused = jnp.full((N_SEQ * 2 * BLK_DEV,), -1, jnp.int32)
    return (unused.at[slot_all].set(image_all), unused.at[slot_all].set(view_all))


def draw_slot_image(key, part):
    return slot_layout(key)[0]


def draw_slot_dest(key, part):
    return slot_layout(key)[1]


def draw_w_qkv(key, part):
    key_parts = jax.random.split(jax.random.fold_in(key, 77), 1)
    spread = D ** (-0.5)
    weights = jax.random.normal(key_parts[0], (3, D, D), jnp.float32) * spread
    return jnp.clip(weights, -1.15, 1.15).astype(jnp.bfloat16)


def block_scale(own_key, shape, cuts, smallest, largest):
    factor_of = 1.0
    for position, shards_of in cuts:
        steps = jax.random.uniform(jax.random.fold_in(jax.random.fold_in(own_key, 6), position), (shards_of,), jnp.float32, smallest / len(cuts), largest / len(cuts))
        factor_of = factor_of * jnp.repeat(jnp.exp(steps), shape[position] // shards_of).reshape((-1,) + (1,) * (len(shape) - 1 - position))
    return factor_of


def scatter_about(rng, shape, scale, reach, shards=(), kind=jnp.bfloat16):
    array = scale * jax.random.normal(rng, shape, jnp.float32)
    if shards:
        array = array * block_scale(rng, shape, shards, -0.22, 0.18)
    return jnp.clip(array, -reach, reach).astype(kind)


def setup_inputs(seed: int = 0) -> dict:
    seeds = jax.random.split(jax.random.key(seed), 12)
    return {
        "patches": scatter_about(seeds[0], (WTOKENS, D), 1.0, 6.0, ((0, 8),)),
        "slot_image": draw_slot_image(jax.random.fold_in(seeds[11], 71), 0),
        "slot_dest": draw_slot_dest(jax.random.fold_in(seeds[11], 71), 0),
        "enc_gain": jnp.clip(1.0 + 0.18 * jax.random.normal(seeds[3], (D,), jnp.float32), 0.1, 1.9),
        "w_qkv": draw_w_qkv(jax.random.fold_in(seeds[11], 71), 0),
        "w_out": scatter_about(seeds[5], (D, D), D ** -0.5, 0.21875, ((0, 4),)),
        "fast_gain": jnp.clip(1.0 + 0.18 * jax.random.normal(seeds[6], (D,), jnp.float32), 0.1, 1.9),
        "w_fast": scatter_about(seeds[7], (3, D, D), D ** -0.5, 0.21875, ((2, 4),)),
        "w_rate": scatter_about(seeds[8], (D, FHEADS), D ** -0.5, 0.21875, ((1, 4),)),
        "fast_gate_up": scatter_about(seeds[9], (FHEADS, 2, FW, FH), FW ** -0.5, 0.4375, ((0, 4),), jnp.float32),
        "fast_down": scatter_about(seeds[10], (FHEADS, FH, FW), FH ** -0.5, 0.3125, ((0, 4),), jnp.float32),
    }


EPSILON = 1e-06
RATE_SCALE = 0.1

def norm_rows(values, gain_vector):
    widened = values.astype(jnp.float32)
    factor = lax.rsqrt(lax.optimization_barrier(jnp.mean(widened * widened, axis=-1, keepdims=True)) + EPSILON)
    return (widened * factor * gain_vector.astype(jnp.float32)).astype(jnp.bfloat16)

def attend_pair(pieces):
    query_rows, key_rows, value_rows, token_ids = pieces
    token_count = query_rows.shape[0]
    heads_here = query_rows.shape[1] // HDIM
    q_heads = query_rows.astype(jnp.float32).reshape(token_count, heads_here, HDIM)
    k_heads = key_rows.astype(jnp.float32).reshape(token_count, heads_here, HDIM)
    v_heads = value_rows.astype(jnp.float32).reshape(token_count, heads_here, HDIM)
    scores = jnp.einsum('qhe,khe->hqk', q_heads, k_heads) * HDIM ** (-0.5)
    allowed = token_ids[:, None] == token_ids[None, :]
    scores = jnp.where(allowed[None], scores, -1e+30)
    top_score = lax.optimization_barrier(jnp.max(scores, axis=-1, keepdims=True))
    exp_scores = jnp.exp(scores - top_score)
    weights = (exp_scores / lax.optimization_barrier(jnp.sum(exp_scores, axis=-1, keepdims=True))).astype(jnp.bfloat16)
    mixed_heads = jnp.einsum('hqk,khe->qhe', weights.astype(jnp.float32), v_heads)
    return mixed_heads.astype(jnp.bfloat16).reshape(token_count, heads_here * HDIM)

def encode_group(rows_here, ids_here, enc_gain, w_qkv, w_out):
    normed = norm_rows(rows_here, enc_gain)
    projected = [jnp.dot(normed, w_qkv[which_one], preferred_element_type=jnp.float32).astype(jnp.bfloat16) for which_one in range(3)]
    span = 2 * BLK
    pair_count = rows_here.shape[0] // span
    attended = lax.map(attend_pair, (projected[0].reshape(pair_count, span, D), projected[1].reshape(pair_count, span, D), projected[2].reshape(pair_count, span, D), ids_here.reshape(pair_count, span)))
    attended = attended.reshape(rows_here.shape[0], D)
    head_total = jnp.zeros((rows_here.shape[0], D), jnp.float32)
    for group_index in range(FHEADS):
        block_cols = attended[:, group_index * FW:(group_index + 1) * FW]
        product = jnp.dot(block_cols, w_out[group_index * FW:(group_index + 1) * FW], preferred_element_type=jnp.float32)
        rounded = lax.optimization_barrier(product.astype(jnp.bfloat16))
        head_total = head_total + rounded.astype(jnp.float32)
    return (rows_here.astype(jnp.float32) + head_total).astype(jnp.bfloat16)

def renorm(updated, initial):
    target_norm = jnp.sqrt(lax.optimization_barrier(jnp.sum(initial * initial, axis=1, keepdims=True)))
    return updated * target_norm * lax.rsqrt(lax.optimization_barrier(jnp.sum(updated * updated, axis=1, keepdims=True)) + EPSILON)

def reference(patches, slot_image, slot_dest, enc_gain, w_qkv, w_out, fast_gain, w_fast, w_rate, fast_gate_up, fast_down):
    view_count = N_SEQ * BLK_DEV
    slot_total = N_SEQ * WSLOT
    target = jnp.where(slot_dest >= 0, slot_dest, view_count).astype(jnp.int32)
    view_blocks = jnp.zeros((view_count + 1, BLK, D), patches.dtype).at[target].set(patches.reshape(slot_total, BLK, D))[:view_count]
    view_ids = jnp.zeros((view_count + 1,), jnp.int32).at[target].set(slot_image.astype(jnp.int32))[:view_count]
    pair_total = view_count // 2
    group_size = math.gcd(8, pair_total)
    group_rows = view_blocks.reshape(pair_total // group_size, group_size * 2 * BLK, D)
    group_ids = jnp.repeat(view_ids, BLK).reshape(pair_total // group_size, group_size * 2 * BLK)
    embedded = lax.map(lambda pieces: encode_group(pieces[0], pieces[1], enc_gain, w_qkv, w_out), (group_rows, group_ids))
    embedded = embedded.reshape(view_count * BLK, D)
    normed_fast = norm_rows(embedded, fast_gain)
    fast_query = jnp.dot(normed_fast, w_fast[0], preferred_element_type=jnp.float32).astype(jnp.bfloat16)
    fast_key = jnp.dot(normed_fast, w_fast[1], preferred_element_type=jnp.float32).astype(jnp.bfloat16)
    fast_value = jnp.dot(normed_fast, w_fast[2], preferred_element_type=jnp.float32).astype(jnp.bfloat16)
    rate_all = RATE_SCALE * jax.nn.softplus(jnp.dot(normed_fast, w_rate, preferred_element_type=jnp.float32)) * VTOKENS ** (-0.5)
    columns_out = []
    for fast_head in range(FHEADS):
        chosen = slice(fast_head * FW, (fast_head + 1) * FW)
        key_here = fast_key[:, chosen]
        query_here = fast_query[:, chosen]
        gate_init = fast_gate_up[fast_head, 0]
        up_init = fast_gate_up[fast_head, 1]
        down_init = fast_down[fast_head]
        gate_half = gate_init.astype(jnp.bfloat16)
        up_half = up_init.astype(jnp.bfloat16)
        down_half = down_init.astype(jnp.bfloat16)
        key_gate = jnp.dot(key_here, gate_half, preferred_element_type=jnp.float32)
        key_up = jnp.dot(key_here, up_half, preferred_element_type=jnp.float32)
        hidden_key = (jax.nn.silu(key_gate) * key_up).astype(jnp.bfloat16)
        out_grad = (-rate_all[:, fast_head:fast_head + 1] * fast_value[:, chosen].astype(jnp.float32)).astype(jnp.bfloat16)
        grad_down = jnp.dot(hidden_key.T, out_grad, preferred_element_type=jnp.float32)
        hidden_grad = jnp.dot(out_grad, down_half.T, preferred_element_type=jnp.float32)
        sigmoid_gate = jax.nn.sigmoid(key_gate)
        gate_grad = (hidden_grad * key_up * sigmoid_gate * (1.0 + key_gate * (1.0 - sigmoid_gate))).astype(jnp.bfloat16)
        up_grad = (hidden_grad * jax.nn.silu(key_gate)).astype(jnp.bfloat16)
        grad_gate = jnp.dot(key_here.T, gate_grad, preferred_element_type=jnp.float32)
        grad_up = jnp.dot(key_here.T, up_grad, preferred_element_type=jnp.float32)
        applied_gate = renorm(gate_init - grad_gate, gate_init).astype(jnp.bfloat16)
        applied_up = renorm(up_init - grad_up, up_init).astype(jnp.bfloat16)
        applied_down = renorm(down_init - grad_down, down_init).astype(jnp.bfloat16)
        query_gate = jnp.dot(query_here, applied_gate, preferred_element_type=jnp.float32)
        query_up = jnp.dot(query_here, applied_up, preferred_element_type=jnp.float32)
        query_hidden = (jax.nn.silu(query_gate) * query_up).astype(jnp.bfloat16)
        fast_out = jnp.dot(query_hidden, applied_down, preferred_element_type=jnp.float32)
        columns_out.append((embedded[:, chosen].astype(jnp.float32) + fast_out).astype(jnp.bfloat16))
    return jnp.concatenate(columns_out, axis=1)
```

```python
import functools

import jax
import jax.numpy as jnp
from jax import lax
from jax.experimental import pallas as pl
from jax.experimental.pallas import tpu as pltpu
from jax.sharding import PartitionSpec as P

HDIM = 64
BLK = 256
BLK_DEV = 8
PAIR = 2 * BLK
EPSILON = 1e-06
RATE_SCALE = 0.1
LANES = 128
MESH = pl.DeviceIdType.MESH
VMEM = pl.BlockSpec(memory_space=pltpu.VMEM)
NT = (((1,), (1,)), ((), ()))


def remote(src, dst, send, recv, device):
    return pltpu.make_async_remote_copy(
        src_ref=src, dst_ref=dst, send_sem=send, recv_sem=recv, device_id=device, device_id_type=MESH
    )


def comm_params(number):
    return pltpu.CompilerParams(
        collective_id=number, has_side_effects=True, vmem_limit_bytes=56 * 1024 * 1024
    )


def greet(devices):
    barrier = pltpu.get_barrier_semaphore()
    for device in devices:
        pl.semaphore_signal(barrier, inc=1, device_id=device, device_id_type=MESH)
    pl.semaphore_wait(barrier, len(devices))


def others(axis_size, me):
    return [lax.rem(me + step, axis_size) for step in range(1, axis_size)]


def head_pals(head_count, head):
    partner = head + 1 - 2 * lax.rem(head, 2)
    peer = lax.rem(head + head_count // 2, head_count)
    return partner, peer


def entry_kernel(n, nh, x_ref, m_ref, w_ref, ox, om, ow, sx, rx, sm, rm, sw, rw):
    seq, head = lax.axis_index("seq"), lax.axis_index("head")
    partner, peer = head_pals(nh, head)
    across = lax.rem(partner + nh // 2, nh)
    targets = others(n, seq)
    greet([(seq, partner), (seq, peer)] + [(to, head) for to in targets])
    to_peer = remote(w_ref, ow.at[:, head], sw.at[0], rw.at[0], (seq, peer))
    to_partner = remote(w_ref, ow.at[:, head], sw.at[1], rw.at[1], (seq, partner))
    to_peer.start()
    to_partner.start()
    copies = []
    for step, to in enumerate(targets):
        copies.append(remote(m_ref.at[to], om.at[seq], sm.at[step], rm.at[step], (to, head)))
        copies.append(remote(x_ref.at[to], ox.at[seq], sx.at[step], rx.at[step], (to, head)))
    for copy in copies:
        copy.start()
    ox[seq] = x_ref[seq]
    om[seq] = m_ref[seq]
    for part in range(w_ref.shape[0]):
        ow[part, head] = w_ref[part]
    to_peer.wait_recv()
    forward = remote(ow.at[:, peer], ow.at[:, peer], sw.at[2], rw.at[2], (seq, partner))
    forward.start()
    to_peer.wait_send()
    to_partner.wait()
    for copy in copies:
        copy.wait()
    forward.wait()


def enter(rows, meta, weights, n, nh):
    dma = pltpu.SemaphoreType.DMA
    return pl.pallas_call(
        functools.partial(entry_kernel, n, nh),
        out_shape=(
            jax.ShapeDtypeStruct(rows.shape, rows.dtype),
            jax.ShapeDtypeStruct(meta.shape, meta.dtype),
            jax.ShapeDtypeStruct(
                (weights.shape[0], nh) + weights.shape[1:], weights.dtype
            ),
        ),
        in_specs=[VMEM] * 3,
        out_specs=(VMEM,) * 3,
        scratch_shapes=[
            dma((n - 1,)), dma((n - 1,)), dma((n - 1,)), dma((n - 1,)), dma((3,)), dma((3,)),
        ],
        compiler_params=comm_params(1),
        name="entry_exchange",
    )(rows, meta, weights)


def swap_kernel(nh, x_ref, o_ref, send, recv):
    seq, head = lax.axis_index("seq"), lax.axis_index("head")
    targets = others(nh, head)
    greet([(seq, to) for to in targets])
    copies = [
        remote(x_ref.at[to], o_ref.at[head], send.at[step], recv.at[step], (seq, to))
        for step, to in enumerate(targets)
    ]
    for copy in copies:
        copy.start()
    o_ref[head] = x_ref[head]
    for copy in copies:
        copy.wait()


def head_swap(x, nh):
    dma = pltpu.SemaphoreType.DMA
    return pl.pallas_call(
        functools.partial(swap_kernel, nh),
        out_shape=jax.ShapeDtypeStruct(x.shape, x.dtype),
        in_specs=[VMEM],
        out_specs=VMEM,
        scratch_shapes=[dma((nh - 1,)), dma((nh - 1,))],
        compiler_params=comm_params(2),
        name="head_swap",
    )(x)


def route_kernel(nh, dest_ref, image_ref, x_ref, o_ref, m_ref, sems):
    head = lax.axis_index("head")
    part = o_ref.shape[1]
    pairs = dest_ref.shape[0] // 2
    m_ref[...] = jnp.full(m_ref.shape, -1, jnp.int32)

    def piece(pair):
        dest = dest_ref[2 * pair]
        known = jnp.maximum(dest, 0)
        offset = head * part
        slot = 2 * pair + lax.rem(known + lax.div(offset, BLK), 2)
        start = pl.multiple_of(slot * BLK + lax.rem(offset, BLK), part)
        target = lax.div(known, BLK_DEV)
        copy = pltpu.make_async_copy(x_ref.at[pl.ds(start, part)], o_ref.at[target], sems.at[pair])
        return dest, target, copy

    for pair in range(pairs):
        dest, target, copy = piece(pair)

        @pl.when(dest >= 0)
        def _():
            copy.start()
            same = (image_ref[2 * pair] == image_ref[2 * pair + 1]).astype(jnp.int32)
            code = 2 * lax.div(lax.rem(dest, BLK_DEV), 2) + same
            m_ref[target] = jnp.full(m_ref.shape[1:], code, jnp.int32)

    for pair in range(pairs):
        dest, target, copy = piece(pair)

        @pl.when(dest >= 0)
        def _():
            copy.wait()


def route(slot_dest, slot_image, patches, n, nh):
    smem = pl.BlockSpec(memory_space=pltpu.SMEM)
    part = PAIR // nh
    return pl.pallas_call(
        functools.partial(route_kernel, nh),
        out_shape=(
            jax.ShapeDtypeStruct((n, part, patches.shape[1]), patches.dtype),
            jax.ShapeDtypeStruct((n, 8, LANES), jnp.int32),
        ),
        in_specs=[smem, smem, pl.BlockSpec(memory_space=pl.ANY)],
        out_specs=(VMEM, VMEM),
        scratch_shapes=[pltpu.SemaphoreType.DMA((slot_dest.shape[0] // 2,))],
        compiler_params=pltpu.CompilerParams(vmem_limit_bytes=56 * 1024 * 1024),
        name="route_pairs",
    )(slot_dest, slot_image, patches)


def select_kernel(code_ref, x_ref, o_ref, same_ref, sems):
    head = lax.axis_index("head")
    same_ref[0] = 0

    def begin(source, carry):
        code = code_ref[source]

        @pl.when(code >= 0)
        def _():
            pair = lax.div(code, 2)
            pltpu.make_async_copy(x_ref.at[source], o_ref.at[pair], sems.at[pair]).start()

            @pl.when(pair == head)
            def _():
                same_ref[0] = lax.rem(code, 2)

        return carry

    lax.fori_loop(0, code_ref.shape[0], begin, 0)
    for pair in range(o_ref.shape[0]):
        pltpu.make_async_copy(x_ref.at[0], o_ref.at[pair], sems.at[pair]).wait()


def select(codes, arrived, pairs):
    smem = pl.BlockSpec(memory_space=pltpu.SMEM)
    return pl.pallas_call(
        select_kernel,
        out_shape=(
            jax.ShapeDtypeStruct((pairs,) + arrived.shape[1:], arrived.dtype),
            jax.ShapeDtypeStruct((1,), jnp.int32),
        ),
        in_specs=[smem, pl.BlockSpec(memory_space=pl.ANY)],
        out_specs=(VMEM, smem),
        scratch_shapes=[pltpu.SemaphoreType.DMA((pairs,))],
        compiler_params=pltpu.CompilerParams(vmem_limit_bytes=24 * 1024 * 1024),
        name="select_pairs",
    )(codes, arrived)


CHUNK = 128


def encode_kernel(
    nh, flag_ref, x_ref, w_ref, gain_ref, o_ref, q_ref, k_ref, v_ref, a_ref, send, recv
):
    seq, head = lax.axis_index("seq"), lax.axis_index("head")
    partner, peer = head_pals(nh, head)
    greet([(seq, partner), (seq, peer)])
    width = x_ref.shape[1]
    wide = x_ref[...].astype(jnp.float32)
    factor = lax.rsqrt(jnp.mean(wide * wide, axis=-1, keepdims=True) + EPSILON)
    normed = (wide * factor * gain_ref[...]).astype(jnp.bfloat16)

    def project(which):
        return lax.dot_general(
            normed, w_ref[which].reshape(width, width), NT, preferred_element_type=jnp.float32
        ).astype(jnp.bfloat16)

    q_ref[...] = project(0) * jnp.bfloat16(HDIM ** (-0.5))
    k_ref[...] = project(1)
    v_ref[...] = project(2)
    apart = jnp.where(flag_ref[0] > 0, 0.0, -1e30).astype(jnp.float32)
    key_block = lax.broadcasted_iota(jnp.int32, (1, PAIR), 1) // BLK
    first = lax.broadcasted_iota(jnp.int32, (CHUNK, LANES), 1) < HDIM
    direct = []
    forwards = []

    for chunk in range(PAIR // CHUNK):
        rows = pl.ds(chunk * CHUNK, CHUNK)
        bias = jnp.where(key_block == chunk * CHUNK // BLK, 0.0, apart)

        def slabs(index, carry):
            for inner in range(2):
                columns = pl.ds(pl.multiple_of((2 * index + inner) * LANES, LANES), LANES)
                query = q_ref[rows, columns]
                nothing = jnp.zeros_like(query)
                both = jnp.concatenate(
                    [jnp.where(first, query, nothing), jnp.where(first, nothing, query)], axis=0
                )
                scores = lax.dot_general(
                    both, k_ref[:, columns], NT, preferred_element_type=jnp.float32
                ) + bias
                top = jnp.max(scores, axis=-1, keepdims=True)
                weights = jnp.exp(scores - top)
                total = jnp.sum(weights, axis=-1, keepdims=True)
                mixed = jnp.dot(
                    weights.astype(jnp.bfloat16),
                    v_ref[:, columns],
                    preferred_element_type=jnp.float32,
                ) * (1.0 / total)
                a_ref[:, columns] = jnp.where(first, mixed[:CHUNK], mixed[CHUNK:]).astype(
                    jnp.bfloat16
                )
            return carry

        lax.fori_loop(0, width // LANES // 2, slabs, 0)
        mixed = jnp.dot(
            a_ref[...], w_ref[3].reshape(width, width), preferred_element_type=jnp.float32
        )
        o_ref[head, rows] = (x_ref[rows].astype(jnp.float32) + mixed).astype(jnp.bfloat16)
        mine = o_ref.at[head, rows]
        to_peer = remote(mine, mine, send.at[0, chunk], recv.at[0, chunk], (seq, peer))
        to_partner = remote(mine, mine, send.at[1, chunk], recv.at[1, chunk], (seq, partner))
        to_peer.start()
        to_partner.start()
        direct.append((to_peer, to_partner))
    for chunk, (to_peer, to_partner) in enumerate(direct):
        to_peer.wait_recv()
        theirs = o_ref.at[peer, pl.ds(chunk * CHUNK, CHUNK)]
        forward = remote(theirs, theirs, send.at[2, chunk], recv.at[2, chunk], (seq, partner))
        forward.start()
        forwards.append(forward)
    for (to_peer, to_partner), forward in zip(direct, forwards):
        to_peer.wait_send()
        to_partner.wait()
        forward.wait()


def encode_and_gather(flag, rows, weights, gain, nh):
    dma = pltpu.SemaphoreType.DMA
    chunks = PAIR // CHUNK
    return pl.pallas_call(
        functools.partial(encode_kernel, nh),
        out_shape=jax.ShapeDtypeStruct((nh,) + rows.shape, rows.dtype),
        in_specs=[pl.BlockSpec(memory_space=pltpu.SMEM), VMEM, VMEM, VMEM],
        out_specs=VMEM,
        scratch_shapes=[pltpu.VMEM(rows.shape, jnp.bfloat16)] * 3
        + [pltpu.VMEM((CHUNK, rows.shape[1]), jnp.bfloat16), dma((3, chunks)), dma((3, chunks))],
        compiler_params=comm_params(3),
        name="encode_and_gather",
    )(flag, rows, weights, gain)


UNIT = 256
TT = (((0,), (0,)), ((), ()))


def dot(a, b):
    return jnp.dot(a, b, preferred_element_type=jnp.float32)


def dot_nt(a, b):
    return lax.dot_general(a, b, NT, preferred_element_type=jnp.float32)


def renorm(updated, initial, axis):
    target_norm = jnp.sqrt(jnp.sum(initial * initial, axis=axis, keepdims=True))
    return (
        updated
        * target_norm
        * lax.rsqrt(jnp.sum(updated * updated, axis=axis, keepdims=True) + EPSILON)
    )


def fast_kernel(
    n, e_ref, wf_ref, wr_ref, gu_ref, dn_ref, gain_ref, o_ref,
    w_s, q_s, k_s, kt_s, og_s, ogt_s, col_s, pair_s, hk_s, guw_s, dnh_s, dn_s, g_s, sum_s, ag_s, ad_s,
    part_s, xin_s, half_s, zin_s, res_s,
    xs, xr, zs, zr, rs, rr, fs, fr,
):
    seq, head = lax.axis_index("seq"), lax.axis_index("head")
    inner_count, outer_count = 2, n // 2
    inner, outer = lax.rem(seq, 2), lax.div(seq, 2)
    side = (outer * 2 + 1 - inner, head)
    lane = [(lax.rem(outer + step, outer_count) * 2 + inner, head) for step in range(1, outer_count)]
    greet([side] + lane)
    tokens, model = e_ref.shape
    width, hidden = gu_ref.shape[1:]
    wide = k_s.shape[1]
    parts = hidden // LANES
    chunk = part_s.shape[3]
    bf, f32 = jnp.bfloat16, jnp.float32

    w_s[...] = jnp.zeros_like(w_s)
    for which in range(3):
        w_s[:, which * wide : which * wide + width] = wf_ref[which]
    rate_at = 2 * wide + width
    w_s[:, rate_at : rate_at + 1] = wr_ref[...]
    guw_s[...] = jnp.zeros_like(guw_s)
    dnh_s[...] = jnp.zeros_like(dnh_s)
    dn_s[...] = jnp.zeros_like(dn_s)
    dn_s[:, :width] = dn_ref[...]
    dnh_s[...] = dn_s[...].astype(bf)
    g_s[...] = jnp.zeros_like(g_s)
    for part in range(parts):
        cut = slice(part * LANES, (part + 1) * LANES)
        guw_s[part, :width, :LANES] = gu_ref[0, :, cut].astype(bf)
        guw_s[part, :width, LANES:] = gu_ref[1, :, cut].astype(bf)

    for which in range(model // width):

        @pl.when(head == which)
        def _():
            col_s[...] = e_ref[:, which * width : (which + 1) * width]

    token_total = tokens * n

    def project(unit, carry):
        rows = pl.ds(pl.multiple_of(unit * UNIT, UNIT), UNIT)
        wide_rows = e_ref[rows].astype(f32)
        factor = lax.rsqrt(jnp.mean(wide_rows * wide_rows, axis=-1, keepdims=True) + EPSILON)
        normed = (wide_rows * factor * gain_ref[...]).astype(bf)
        mapped = dot(normed, w_s[...])
        q_s[rows] = mapped[:, :wide].astype(bf)
        key = mapped[:, wide : 2 * wide].astype(bf)
        k_s[rows] = key
        kt_s[:, rows] = key.T
        value = mapped[:, 2 * wide :].astype(bf).astype(f32)
        before = mapped[:, rate_at : rate_at + 1]
        soft = jnp.maximum(before, 0.0) + jnp.log1p(jnp.exp(-jnp.abs(before)))
        rate = (RATE_SCALE * token_total ** (-0.5)) * soft
        back = (-rate * value).astype(bf)
        og_s[rows] = back
        ogt_s[:, rows] = back.T
        return carry

    lax.fori_loop(0, tokens // UNIT, project, 0)

    def compute(part):
        def body(unit, carry):
            rows = pl.ds(pl.multiple_of(unit * UNIT, UNIT), UNIT)
            both = dot(k_s[rows], guw_s[part])
            gate, up = both[:, :LANES], both[:, LANES:]
            grad = dot_nt(og_s[rows], dnh_s[part * LANES : (part + 1) * LANES])
            sig = jax.nn.sigmoid(gate)
            silu = gate * sig
            hk_s[rows] = (silu * up).astype(bf)
            pair_s[rows, :LANES] = (grad * up * sig * (1.0 + gate * (1.0 - sig))).astype(bf)
            pair_s[rows, LANES:] = (grad * silu).astype(bf)
            return carry

        lax.fori_loop(0, tokens // UNIT, body, 0)
        first = dot(kt_s[...], pair_s[...])
        second = dot(ogt_s[...], hk_s[...])
        g_s[0:width] = first[:width, :LANES]
        g_s[width : 2 * width] = first[:width, LANES:]
        g_s[2 * width : 3 * width] = second[:width]
        for i in range(inner_count):
            for o in range(outer_count):
                at = (i * outer_count + o) * chunk
                part_s[part, i, o] = g_s[at : at + chunk].astype(bf)

    def x_copy(part):
        return remote(part_s.at[part, 1 - inner], xin_s.at[part], xs.at[part], xr.at[part], side)

    def z_copies(part):
        return [
            remote(
                half_s.at[part, lax.rem(outer + step, outer_count)], zin_s.at[part, step - 1],
                zs.at[part, step - 1], zr.at[part, step - 1], lane[step - 1],
            )
            for step in range(1, outer_count)
        ]

    def r_copies(part):
        mine = res_s.at[part, inner, outer]
        return [
            remote(mine, mine, rs.at[part, step], rr.at[part, step], to)
            for step, to in enumerate(lane + [side])
        ]

    def f_copy(part, step):
        theirs = res_s.at[part, inner, lax.rem(outer + outer_count - step, outer_count)]
        return remote(theirs, theirs, fs.at[part, step - 1], fr.at[part, step - 1], side)

    def stage_x(part):
        x_copy(part).start()

    def stage_z(part):
        x_copy(part).wait_recv()
        for o in range(outer_count):
            half_s[part, o] = (
                part_s[part, inner, o].astype(f32) + xin_s[part, o].astype(f32)
            ).astype(bf)
        for copy in z_copies(part):
            copy.start()

    def stage_r(part):
        total = half_s[part, outer].astype(f32)
        for step, copy in enumerate(z_copies(part)):
            copy.wait_recv()
            total = total + zin_s[part, step].astype(f32)
        res_s[part, inner, outer] = total.astype(bf)
        for copy in r_copies(part):
            copy.start()

    def stage_f(part):
        copies = r_copies(part)
        for step in range(1, outer_count):
            copies[step - 1].wait_recv()
            f_copy(part, step).start()

    def finish(part):
        r_copies(part)[-1].wait_recv()
        for step in range(1, outer_count):
            f_copy(part, step).wait_recv()

    stages = [stage_x, stage_z, stage_r, stage_f]
    for tick in range(parts + len(stages) - 1):
        if tick < parts:
            compute(tick)
        for which, stage in enumerate(stages):
            if 0 <= tick - which < parts:
                stage(tick - which)
    for part in range(parts):
        finish(part)
        cut = slice(part * LANES, (part + 1) * LANES)
        for i in range(inner_count):
            for o in range(outer_count):
                at = (i * outer_count + o) * chunk
                sum_s[at : at + chunk, cut] = res_s[part, i, o].astype(f32)
    for part in range(parts):
        x_copy(part).wait_send()
        for copy in z_copies(part) + r_copies(part):
            copy.wait_send()
        for step in range(1, outer_count):
            f_copy(part, step).wait_send()

    ag_s[...] = jnp.zeros_like(ag_s)
    for which in range(2):
        start = gu_ref[which]
        fresh = renorm(start - sum_s[which * width : (which + 1) * width], start, 1)
        ag_s[:width, which * hidden : (which + 1) * hidden] = fresh.astype(bf)
    start = dn_s[...].T[:width]
    ad_s[...] = renorm(start - sum_s[2 * width : 3 * width], start, 0).astype(bf)

    def final(unit, carry):
        rows = pl.ds(pl.multiple_of(unit * UNIT, UNIT), UNIT)
        both = dot(q_s[rows], ag_s[...])
        gate = both[:, :hidden]
        inside = (gate * jax.nn.sigmoid(gate) * both[:, hidden:]).astype(bf)
        o_ref[rows] = (col_s[rows].astype(f32) + dot_nt(inside, ad_s[...])).astype(bf)
        return carry

    lax.fori_loop(0, tokens // UNIT, final, 0)


def fast_update(embedded, w_fast, w_rate, gate_up, down, gain, n):
    tokens, model = embedded.shape
    width, hidden = gate_up.shape[1:]
    wide = LANES * (-(-width // LANES))
    parts = hidden // LANES
    chunk = 8 * (-(-3 * width // (8 * n)))
    rows = max(3 * width, chunk * n)
    bf, f32 = jnp.bfloat16, jnp.float32
    vmem, dma = pltpu.VMEM, pltpu.SemaphoreType.DMA
    outer = n // 2
    return pl.pallas_call(
        functools.partial(fast_kernel, n),
        out_shape=jax.ShapeDtypeStruct((tokens, width), bf),
        in_specs=[VMEM] * 6,
        out_specs=VMEM,
        scratch_shapes=[
            vmem((model, 3 * wide), bf),
            vmem((tokens, wide), bf), vmem((tokens, wide), bf), vmem((wide, tokens), bf),
            vmem((tokens, wide), bf), vmem((wide, tokens), bf), vmem((tokens, width), bf),
            vmem((tokens, 2 * LANES), bf), vmem((tokens, LANES), bf),
            vmem((parts, wide, 2 * LANES), bf), vmem((hidden, wide), bf), vmem((hidden, wide), f32),
            vmem((rows, LANES), f32), vmem((rows, hidden), f32),
            vmem((wide, 2 * hidden), bf), vmem((width, hidden), bf),
            vmem((parts, 2, outer, chunk, LANES), bf), vmem((parts, outer, chunk, LANES), bf),
            vmem((parts, outer, chunk, LANES), bf), vmem((parts, outer - 1, chunk, LANES), bf),
            vmem((parts, 2, outer, chunk, LANES), bf),
            dma((parts,)), dma((parts,)), dma((parts, outer - 1)), dma((parts, outer - 1)),
            dma((parts, outer)), dma((parts, outer)), dma((parts, outer - 1)), dma((parts, outer - 1)),
        ],
        compiler_params=comm_params(4),
        name="fast_update",
    )(embedded, w_fast, w_rate, gate_up, down, gain)


def on_device(
    patches,
    slot_image,
    slot_dest,
    enc_gain,
    w_qkv,
    w_out,
    fast_gain,
    w_fast,
    w_rate,
    fast_gate_up,
    fast_down,
):
    n = lax.axis_size("seq")
    nh = lax.axis_size("head")
    head = lax.axis_index("head")
    model = patches.shape[1]
    sending, meta = route(slot_dest, slot_image, patches, n, nh)
    weights = jnp.concatenate([jnp.swapaxes(w_qkv, 1, 2), w_out[None]], axis=0)
    arrived, codes, full_weights = enter(sending, meta, weights, n, nh)
    chosen, same = select(codes[:, 0, 0], arrived, BLK_DEV // 2)
    own_pair = head_swap(chosen, nh).reshape(PAIR, model)
    full_embedded = encode_and_gather(same, own_pair, full_weights, enc_gain[None, :], nh)
    full_embedded = full_embedded.reshape(nh * PAIR, model)
    return fast_update(
        full_embedded, w_fast, w_rate, fast_gate_up[0], fast_down[0], fast_gain[None, :], n
    )


def solution(mesh):
    in_specs = (
        P("seq", None),
        P("seq"),
        P("seq"),
        P(),
        P(None, None, "head"),
        P("head", None),
        P(),
        P(None, None, "head"),
        P(None, "head"),
        P("head", None, None, None),
        P("head", None, None),
    )
    out_specs = P("seq", "head")
    return jax.shard_map(
        on_device, mesh=mesh, in_specs=in_specs, out_specs=out_specs, check_vma=False
    )
```

```python
import functools
import types

import jax
import jax.numpy as jnp
from jax import lax
from jax.experimental import pallas as pl
from jax.experimental.pallas import tpu as pltpu
from jax.sharding import PartitionSpec as P

HDIM = 64
BLK = 256
BLK_DEV = 8
PAIR = 2 * BLK
EPSILON = 1e-06
RATE_SCALE = 0.1
LANES = 128
STEPS = 4
CHUNK = 128
UNIT = 256
MESH = pl.DeviceIdType.MESH
VMEM = pl.BlockSpec(memory_space=pltpu.VMEM)
SMEM = pl.BlockSpec(memory_space=pltpu.SMEM)
ANY = pl.BlockSpec(memory_space=pl.ANY)
NT = (((1,), (1,)), ((), ()))
BF = jnp.bfloat16
F32 = jnp.float32


def remote(src, dst, send, recv, device):
    return pltpu.make_async_remote_copy(
        src_ref=src, dst_ref=dst, send_sem=send, recv_sem=recv, device_id=device, device_id_type=MESH
    )


def others(axis_size, me):
    return [lax.rem(me + step, axis_size) for step in range(1, axis_size)]


def dot(a, b):
    return jnp.dot(a, b, preferred_element_type=F32)


def dot_nt(a, b):
    return lax.dot_general(a, b, NT, preferred_element_type=F32)


def norm_rows(values, gain):
    wide = values.astype(F32)
    factor = lax.rsqrt(jnp.mean(wide * wide, axis=-1, keepdims=True) + EPSILON)
    return (wide * factor * gain).astype(BF)


def renorm(updated, initial, axis):
    target_norm = jnp.sqrt(jnp.sum(initial * initial, axis=axis, keepdims=True))
    return (
        updated
        * target_norm
        * lax.rsqrt(jnp.sum(updated * updated, axis=axis, keepdims=True) + EPSILON)
    )


def layout(n, nh, slots, model, width, hidden):
    vmem, dma = pltpu.VMEM, pltpu.SemaphoreType.DMA
    part = PAIR // nh
    rows = part // STEPS
    wide = LANES * (-(-width // LANES))
    tokens = nh * PAIR
    parts = hidden // LANES
    chunk = 8 * (-(-3 * width // (8 * n)))
    outer = n // 2
    sizes = {}
    for c in range(STEPS):
        sizes[f"held{c}"] = vmem((slots, rows, model), BF)
        sizes[f"out{c}"] = vmem((n, rows, model), BF)
        sizes[f"in{c}"] = vmem((n, rows, model), BF)
        sizes[f"chosen{c}"] = vmem((nh, rows, model), BF)
    sizes.update(
        meta=vmem((n, 1, LANES), jnp.int32), meta_in=vmem((n, 1, LANES), jnp.int32),
        codes=pltpu.SMEM((n, 1, LANES), jnp.int32),
        w=vmem((4, nh, width, model), BF),
        pair=vmem((2, STEPS, nh // 2, rows, model), BF),
        q=vmem((PAIR, model), BF), k=vmem((PAIR, model), BF), v=vmem((PAIR, model), BF),
        a=vmem((CHUNK, model), BF), emb=vmem((nh, PAIR, model), BF),
        wf_in=vmem((3, width, model), BF), wr_in=vmem((1, model), BF),
        gu=vmem((2, width, hidden), F32), dt=vmem((width, hidden), F32),
        wf=vmem((3 * wide, model), BF), fq=vmem((tokens, wide), BF), fk=vmem((tokens, wide), BF),
        fkt=vmem((wide, tokens), BF), og=vmem((tokens, wide), BF), ogt=vmem((wide, tokens), BF),
        col=vmem((tokens, width), BF), two=vmem((tokens, 2 * LANES), BF), hk=vmem((tokens, LANES), BF),
        guw=vmem((parts, wide, 2 * LANES), BF), dth=vmem((wide, hidden), BF),
        g=vmem((max(3 * width, chunk * n), LANES), F32),
        total=vmem((max(3 * width, chunk * n), hidden), F32),
        ag=vmem((wide, 2 * hidden), BF), ad=vmem((width, hidden), BF),
        part=vmem((parts, 2, outer, chunk, LANES), BF), xin=vmem((parts, outer, chunk, LANES), BF),
        half=vmem((parts, outer, chunk, LANES), BF), zin=vmem((parts, outer - 1, chunk, LANES), BF),
        res=vmem((parts, 2, outer, chunk, LANES), BF),
        local=dma((STEPS + 7,)),
        xs=dma((STEPS, n - 1)), xr=dma((STEPS, n - 1)), ms=dma((n - 1,)), mr=dma((n - 1,)),
        ws=dma((3, 4)), wr=dma((3, 4)), ss=dma((STEPS, nh - 1)), sr=dma((STEPS, nh - 1)),
        gs=dma((3, PAIR // CHUNK)), gr=dma((3, PAIR // CHUNK)),
        ps=dma((parts,)), pr=dma((parts,)), zs=dma((parts, outer - 1)), zr=dma((parts, outer - 1)),
        rs=dma((parts, outer)), rr=dma((parts, outer)),
        fs=dma((parts, outer - 1)), fr=dma((parts, outer - 1)),
    )
    return sizes


def gradient_sum(n, width, s, side, lane, compute, during):
    seq = lax.axis_index("seq")
    outer_count = n // 2
    inner, outer = lax.rem(seq, 2), lax.div(seq, 2)
    parts = s.part.shape[0]
    chunk = s.part.shape[3]
    steps = range(1, outer_count)

    def plan(part):
        mine = s.res.at[part, inner, outer]
        theirs = [s.res.at[part, inner, lax.rem(outer + outer_count - t, outer_count)] for t in steps]
        return types.SimpleNamespace(
            x=remote(s.part.at[part, 1 - inner], s.xin.at[part], s.ps.at[part], s.pr.at[part], side),
            z=[
                remote(
                    s.half.at[part, lax.rem(outer + t, outer_count)], s.zin.at[part, t - 1],
                    s.zs.at[part, t - 1], s.zr.at[part, t - 1], lane[t - 1],
                )
                for t in steps
            ],
            r=[
                remote(mine, mine, s.rs.at[part, t], s.rr.at[part, t], to)
                for t, to in enumerate(lane + [side])
            ],
            f=[
                remote(theirs[t - 1], theirs[t - 1], s.fs.at[part, t - 1], s.fr.at[part, t - 1], side)
                for t in steps
            ],
        )

    plans = [plan(part) for part in range(parts)]

    def stage_x(part):
        plans[part].x.start()

    def stage_z(part):
        plans[part].x.wait_recv()
        for o in range(outer_count):
            s.half[part, o] = (
                s.part[part, inner, o].astype(F32) + s.xin[part, o].astype(F32)
            ).astype(BF)
        for copy in plans[part].z:
            copy.start()

    def stage_r(part):
        total = s.half[part, outer].astype(F32)
        for t, copy in enumerate(plans[part].z):
            copy.wait_recv()
            total = total + s.zin[part, t].astype(F32)
        s.res[part, inner, outer] = total.astype(BF)
        for copy in plans[part].r:
            copy.start()

    def stage_f(part):
        for t in steps:
            plans[part].r[t - 1].wait_recv()
            plans[part].f[t - 1].start()

    stages = [stage_x, stage_z, stage_r, stage_f]
    for tick in range(parts + len(stages) - 1):
        if tick < parts:
            compute(tick)
        for which, stage in enumerate(stages):
            if 0 <= tick - which < parts:
                stage(tick - which)
        if tick == parts - 1:
            during()
    for part in range(parts):
        plans[part].r[-1].wait_recv()
        for copy in plans[part].f:
            copy.wait_recv()
        cut = slice(part * LANES, (part + 1) * LANES)
        for i in range(2):
            for o in range(outer_count):
                at = (i * outer_count + o) * chunk
                s.total[at : at + chunk, cut] = s.res[part, i, o].astype(F32)
    for part in range(parts):
        plans[part].x.wait_send()
        for copy in plans[part].z + plans[part].r + plans[part].f:
            copy.wait_send()


def whole_kernel(
    n, nh, names, dest_ref, image_ref, x_ref, wqkv_ref, wo_ref, eg_ref, fg_ref, wf_ref, wr_ref,
    gu_ref, dt_ref, o_ref, *scratch,
):
    s = types.SimpleNamespace(**dict(zip(names, scratch)))
    seq, head = lax.axis_index("seq"), lax.axis_index("head")
    partner = head + 1 - 2 * lax.rem(head, 2)
    peer = lax.rem(head + nh // 2, nh)
    targets = others(n, seq)
    mates = others(nh, head)
    outer_count = n // 2
    inner, outer = lax.rem(seq, 2), lax.div(seq, 2)
    side = (outer * 2 + 1 - inner, head)
    lane = [(lax.rem(outer + t, outer_count) * 2 + inner, head) for t in range(1, outer_count)]
    model = x_ref.shape[-1]
    width, hidden = gu_ref.shape[1:]
    wide = s.fk.shape[1]
    parts = hidden // LANES
    tokens = nh * PAIR
    held = [getattr(s, f"held{c}") for c in range(STEPS)]
    out = [getattr(s, f"out{c}") for c in range(STEPS)]
    arrived = [getattr(s, f"in{c}") for c in range(STEPS)]
    chosen = [getattr(s, f"chosen{c}") for c in range(STEPS)]
    rows = held[0].shape[1]
    per_block = nh // 2

    barrier = pltpu.get_barrier_semaphore()
    greeted = [(to, head) for to in targets] + [(seq, to) for to in mates]
    for device in greeted:
        pl.semaphore_signal(barrier, inc=1, device_id=device, device_id_type=MESH)

    fetch = [
        pltpu.make_async_copy(x_ref.at[:, lax.rem(head, per_block), c], held[c], s.local.at[c])
        for c in range(STEPS)
    ]
    weights_in = [
        pltpu.make_async_copy(wqkv_ref, s.w.at[0:3, head], s.local.at[STEPS]),
        pltpu.make_async_copy(wo_ref, s.w.at[3, head], s.local.at[STEPS + 1]),
    ]
    late = [
        pltpu.make_async_copy(src, dst, s.local.at[STEPS + 2 + which])
        for which, (src, dst) in enumerate(
            [(wf_ref, s.wf_in), (wr_ref, s.wr_in), (gu_ref, s.gu), (dt_ref, s.dt)]
        )
    ]
    for copy in fetch[:1] + weights_in + fetch[1:] + late:
        copy.start()

    my_block = lax.div(head, per_block)
    pairs = dest_ref.shape[0] // 2
    firsts = [dest_ref[2 * i] for i in range(pairs)]
    sames = [(image_ref[2 * i] == image_ref[2 * i + 1]).astype(jnp.int32) for i in range(pairs)]
    homes = [lax.div(jnp.maximum(d, 0), BLK_DEV) for d in firsts]
    slots = []
    for i, d in enumerate(firsts):
        slots.append(2 * i + lax.rem(jnp.maximum(d, 0) + my_block, 2))
    marks = [
        2 * lax.div(lax.rem(jnp.maximum(d, 0), BLK_DEV), 2) + same for d, same in zip(firsts, sames)
    ]

    def lookup(target):
        slot, code = jnp.int32(0), jnp.int32(-1)
        for i, d in enumerate(firsts):
            hit = jnp.logical_and(d >= 0, homes[i] == target)
            slot = jnp.where(hit, slots[i], slot)
            code = jnp.where(hit, marks[i], code)
        return slot, code

    found = [lookup(to) for to in targets + [seq]]
    for step, to in enumerate(targets):
        s.meta[step] = jnp.full((1, LANES), found[step][1], jnp.int32)
    s.meta_in[seq] = jnp.full((1, LANES), found[-1][1], jnp.int32)

    def pick(c):
        fetch[c].wait()
        for step in range(n - 1):
            out[c][step] = held[c][found[step][0]]
        arrived[c][seq] = held[c][found[-1][0]]

    meta_copies = [
        remote(s.meta.at[step], s.meta_in.at[seq], s.ms.at[step], s.mr.at[step], (to, head))
        for step, to in enumerate(targets)
    ]
    x_copies = [
        [
            remote(out[c].at[step], arrived[c].at[seq], s.xs.at[c, step], s.xr.at[c, step], (to, head))
            for step, to in enumerate(targets)
        ]
        for c in range(STEPS)
    ]
    to_peer = [
        remote(s.w.at[m, head], s.w.at[m, head], s.ws.at[0, m], s.wr.at[0, m], (seq, peer))
        for m in range(4)
    ]
    to_partner = [
        remote(s.w.at[m, head], s.w.at[m, head], s.ws.at[1, m], s.wr.at[1, m], (seq, partner))
        for m in range(4)
    ]
    passed = [
        remote(s.w.at[m, peer], s.w.at[m, peer], s.ws.at[2, m], s.wr.at[2, m], (seq, partner))
        for m in range(4)
    ]
    pick(0)
    pl.semaphore_wait(barrier, len(greeted))
    for copy in meta_copies + x_copies[0]:
        copy.start()
    for copy in weights_in:
        copy.wait()
    for copy in to_peer + to_partner:
        copy.start()
    for c in range(1, STEPS):
        pick(c)
        for copy in x_copies[c]:
            copy.start()

    s.wf[...] = jnp.zeros_like(s.wf)
    s.guw[...] = jnp.zeros_like(s.guw)
    s.dth[...] = jnp.zeros_like(s.dth)
    s.g[...] = jnp.zeros_like(s.g)
    s.ag[...] = jnp.zeros_like(s.ag)
    for copy in late:
        copy.wait()
    for which in range(3):
        s.wf[which * wide : which * wide + width] = s.wf_in[which]
    rate_at = 2 * wide + width
    s.wf[rate_at : rate_at + 16] = jnp.broadcast_to(s.wr_in[...], (16, model))
    s.dth[:width] = s.dt[...].astype(BF)
    for part in range(parts):
        cut = slice(part * LANES, (part + 1) * LANES)
        s.guw[part, :width, :LANES] = s.gu[0, :, cut].astype(BF)
        s.guw[part, :width, LANES:] = s.gu[1, :, cut].astype(BF)

    for copy in meta_copies:
        copy.wait_recv()
    spread = pltpu.make_async_copy(s.meta_in, s.codes, s.local.at[STEPS + 6])
    spread.start()
    spread.wait()
    sources = [jnp.int32(0)] * nh
    same = jnp.int32(0)
    for source in range(n):
        code = s.codes[source, 0, 0]
        place = lax.div(jnp.maximum(code, 0), 2)
        for p in range(nh):
            sources[p] = jnp.where(jnp.logical_and(code >= 0, place == p), source, sources[p])
        mine = jnp.logical_and(code >= 0, place == head)
        same = jnp.where(mine, lax.rem(jnp.maximum(code, 0), 2), same)

    swaps = [
        [
            remote(
                chosen[c].at[to], s.pair.at[lax.div(head, per_block), c, lax.rem(head, per_block)],
                s.ss.at[c, step], s.sr.at[c, step], (seq, to),
            )
            for step, to in enumerate(mates)
        ]
        for c in range(STEPS)
    ]

    def swap(c):
        for copy in x_copies[c]:
            copy.wait_recv()
        for p in range(nh):
            chosen[c][p] = arrived[c][sources[p]]
        for copy in swaps[c]:
            copy.start()
        s.pair[lax.div(head, per_block), c, lax.rem(head, per_block)] = chosen[c][head]

    def matrix(m):
        return s.w[m].reshape(nh * width, model)

    run = per_block * rows

    def project(c):
        for copy in swaps[c]:
            copy.wait_recv()
        taken = jnp.concatenate([s.pair[b, c].reshape(run, model) for b in range(2)], axis=0)
        normed = norm_rows(taken, eg_ref[...])
        for m, ref in enumerate((s.q, s.k, s.v)):
            value = dot_nt(normed, matrix(m)).astype(BF)
            if m == 0:
                value = value * BF(HDIM ** (-0.5))
            for b in range(2):
                at = b * BLK + c * run
                ref[at : at + run] = value[b * run : (b + 1) * run]

    def forward(m):
        to_peer[m].wait_recv()
        passed[m].start()

    for c in range(STEPS):
        swap(c)
        if c == STEPS - 2:
            for m in range(4):
                forward(m)
            for m in range(3):
                to_partner[m].wait_recv()
                passed[m].wait_recv()
            for early in range(c):
                project(early)
    project(STEPS - 2)
    project(STEPS - 1)
    to_partner[3].wait_recv()
    passed[3].wait_recv()

    apart = jnp.where(same > 0, 0.0, -1e30).astype(F32)
    key_block = lax.broadcasted_iota(jnp.int32, (1, PAIR), 1) // BLK
    first = lax.broadcasted_iota(jnp.int32, (CHUNK, LANES), 1) < HDIM
    chunks = PAIR // CHUNK

    def emb_copies(i):
        at = pl.ds(i * CHUNK, CHUNK)
        mine, theirs = s.emb.at[head, at], s.emb.at[peer, at]
        return [
            remote(mine, mine, s.gs.at[0, i], s.gr.at[0, i], (seq, peer)),
            remote(mine, mine, s.gs.at[1, i], s.gr.at[1, i], (seq, partner)),
            remote(theirs, theirs, s.gs.at[2, i], s.gr.at[2, i], (seq, partner)),
        ]

    gathers = [emb_copies(i) for i in range(chunks)]

    def attend(i):
        at = pl.ds(i * CHUNK, CHUNK)
        bias = jnp.where(key_block == i * CHUNK // BLK, 0.0, apart)

        def slabs(index, carry):
            for half in range(2):
                columns = pl.ds(pl.multiple_of((2 * index + half) * LANES, LANES), LANES)
                query = s.q[at, columns]
                nothing = jnp.zeros_like(query)
                both = jnp.concatenate(
                    [jnp.where(first, query, nothing), jnp.where(first, nothing, query)], axis=0
                )
                scores = dot_nt(both, s.k[:, columns]) + bias
                top = jnp.max(scores, axis=-1, keepdims=True)
                weights = jnp.exp(scores - top)
                total = jnp.sum(weights, axis=-1, keepdims=True)
                mixed = dot(weights.astype(BF), s.v[:, columns]) * (1.0 / total)
                s.a[:, columns] = jnp.where(first, mixed[:CHUNK], mixed[CHUNK:]).astype(BF)
            return carry

        lax.fori_loop(0, model // LANES // 2, slabs, 0)
        mixed = dot(s.a[...], matrix(3))
        taken = s.pair[i * CHUNK // BLK].reshape(BLK, model)
        low = i * CHUNK % BLK
        s.emb[head, at] = (taken[low : low + CHUNK].astype(F32) + mixed).astype(BF)
        gathers[i][0].start()
        gathers[i][1].start()

    scale = RATE_SCALE * (tokens * n) ** (-0.5)

    def fast_project(owner, i):
        at = pl.ds(pl.multiple_of(owner * PAIR + i * CHUNK, CHUNK), CHUNK)
        normed = norm_rows(s.emb[owner, pl.ds(i * CHUNK, CHUNK)], fg_ref[...])
        mapped = dot_nt(normed, s.wf[...])
        s.fq[at] = mapped[:, :wide].astype(BF)
        key = mapped[:, wide : 2 * wide].astype(BF)
        s.fk[at] = key
        s.fkt[:, at] = key.T
        value = mapped[:, 2 * wide :].astype(BF).astype(F32)
        before = mapped[:, rate_at : rate_at + 1]
        soft = jnp.maximum(before, 0.0) + jnp.log1p(jnp.exp(-jnp.abs(before)))
        back = (-(scale * soft) * value).astype(BF)
        s.og[at] = back
        s.ogt[:, at] = back.T

    for i in range(chunks):
        attend(i)
        fast_project(head, i)
        if i >= 1:
            gathers[i - 1][0].wait_recv()
            gathers[i - 1][2].start()
    across = lax.rem(partner + nh // 2, nh)
    for i in range(chunks):
        if i == chunks - 1:
            gathers[i][0].wait_recv()
            gathers[i][2].start()
        gathers[i][1].wait_recv()
        fast_project(partner, i)
        fast_project(peer, i)
        gathers[i][2].wait_recv()
        fast_project(across, i)

    def compute(part):
        def body(unit, carry):
            at = pl.ds(pl.multiple_of(unit * UNIT, UNIT), UNIT)
            both = dot(s.fk[at], s.guw[part])
            gate, up = both[:, :LANES], both[:, LANES:]
            grad = dot(s.og[at], s.dth[:, part * LANES : (part + 1) * LANES])
            sig = jax.nn.sigmoid(gate)
            silu = gate * sig
            s.hk[at] = (silu * up).astype(BF)
            s.two[at, :LANES] = (grad * up * sig * (1.0 + gate * (1.0 - sig))).astype(BF)
            s.two[at, LANES:] = (grad * silu).astype(BF)
            return carry

        lax.fori_loop(0, tokens // UNIT, body, 0)
        one = dot(s.fkt[...], s.two[...])
        other = dot(s.ogt[...], s.hk[...])
        s.g[0:width] = one[:width, :LANES]
        s.g[width : 2 * width] = one[:width, LANES:]
        s.g[2 * width : 3 * width] = other[:width]
        chunk = s.part.shape[3]
        for i in range(2):
            for o in range(outer_count):
                at = (i * outer_count + o) * chunk
                s.part[part, i, o] = s.g[at : at + chunk].astype(BF)

    def during():
        for which in range(model // width):

            @pl.when(head == which)
            def _():
                for owner in range(nh):
                    at = owner * PAIR
                    s.col[at : at + PAIR] = s.emb[owner, :, which * width : (which + 1) * width]

    gradient_sum(n, width, s, side, lane, compute, during)

    for which in range(2):
        start = s.gu[which]
        fresh = renorm(start - s.total[which * width : (which + 1) * width], start, 1)
        s.ag[:width, which * hidden : (which + 1) * hidden] = fresh.astype(BF)
    start = s.dt[...]
    s.ad[...] = renorm(start - s.total[2 * width : 3 * width], start, 0).astype(BF)

    def final(unit, carry):
        base = pl.multiple_of(unit * BLK, BLK)
        at = pl.ds(base, BLK)
        both = dot(s.fq[at], s.ag[...])
        gate = both[:, :hidden]
        inside = (gate * jax.nn.sigmoid(gate) * both[:, hidden:]).astype(BF)
        done = (s.col[at].astype(F32) + dot_nt(inside, s.ad[...])).astype(BF)
        for c in range(STEPS):
            for which in range(per_block):
                low = (c * per_block + which) * rows
                to = pl.multiple_of(base + which * STEPS * rows + c * rows, rows)
                o_ref[pl.ds(to, rows)] = done[low : low + rows]
        return carry

    lax.fori_loop(0, tokens // BLK, final, 0)

    for copy in meta_copies + to_peer + to_partner + passed:
        copy.wait_send()
    for group in x_copies + swaps + gathers:
        for copy in group:
            copy.wait_send()


def on_device(
    patches,
    slot_image,
    slot_dest,
    enc_gain,
    w_qkv,
    w_out,
    fast_gain,
    w_fast,
    w_rate,
    fast_gate_up,
    fast_down,
):
    n = lax.axis_size("seq")
    nh = lax.axis_size("head")
    model = patches.shape[1]
    slots = slot_dest.shape[0]
    width, hidden = fast_gate_up.shape[2:]
    part = PAIR // nh
    sizes = layout(n, nh, slots, model, width, hidden)
    return pl.pallas_call(
        functools.partial(whole_kernel, n, nh, tuple(sizes)),
        out_shape=jax.ShapeDtypeStruct((nh * PAIR, width), patches.dtype),
        in_specs=[SMEM, SMEM, ANY, ANY, ANY, VMEM, VMEM, ANY, ANY, ANY, ANY],
        out_specs=VMEM,
        scratch_shapes=list(sizes.values()),
        compiler_params=pltpu.CompilerParams(
            collective_id=1, has_side_effects=True, vmem_limit_bytes=60 * 1024 * 1024
        ),
        name="encode_and_update",
    )(
        slot_dest,
        slot_image,
        patches.reshape(slots, BLK // part, STEPS, part // STEPS, model),
        jnp.swapaxes(w_qkv, 1, 2),
        w_out,
        enc_gain[None, :],
        fast_gain[None, :],
        jnp.swapaxes(w_fast, 1, 2),
        w_rate.T,
        fast_gate_up[0],
        fast_down[0].T,
    )


def solution(mesh):
    in_specs = (
        P("seq", None),
        P("seq"),
        P("seq"),
        P(),
        P(None, None, "head"),
        P("head", None),
        P(),
        P(None, None, "head"),
        P(None, "head"),
        P("head", None, None, None),
        P("head", None, None),
    )
    out_specs = P("seq", "head")
    return jax.shard_map(
        on_device, mesh=mesh, in_specs=in_specs, out_specs=out_specs, check_vma=False
    )
```

```python
import functools
import types

import jax
import jax.numpy as jnp
from jax import lax
from jax.experimental import pallas as pl
from jax.experimental.pallas import tpu as pltpu
from jax.sharding import PartitionSpec as P

HDIM = 64
BLK = 256
BLK_DEV = 8
PAIR = 2 * BLK
EPSILON = 1e-06
RATE_SCALE = 0.1
LANES = 128
STEPS = 4
CHUNK = 128
UNIT = 256
MESH = pl.DeviceIdType.MESH
VMEM = pl.BlockSpec(memory_space=pltpu.VMEM)
SMEM = pl.BlockSpec(memory_space=pltpu.SMEM)
ANY = pl.BlockSpec(memory_space=pl.ANY)
NT = (((1,), (1,)), ((), ()))
BF = jnp.bfloat16
F32 = jnp.float32


def remote(src, dst, send, recv, device):
    return pltpu.make_async_remote_copy(
        src_ref=src, dst_ref=dst, send_sem=send, recv_sem=recv, device_id=device, device_id_type=MESH
    )


def others(axis_size, me):
    return [lax.rem(me + step, axis_size) for step in range(1, axis_size)]


def dot(a, b):
    return jnp.dot(a, b, preferred_element_type=F32)


def dot_nt(a, b):
    return lax.dot_general(a, b, NT, preferred_element_type=F32)


def norm_rows(values, gain):
    wide = values.astype(F32)
    factor = lax.rsqrt(jnp.mean(wide * wide, axis=-1, keepdims=True) + EPSILON)
    return (wide * factor * gain).astype(BF)


def renorm(updated, initial, axis):
    target_norm = jnp.sqrt(jnp.sum(initial * initial, axis=axis, keepdims=True))
    return (
        updated
        * target_norm
        * lax.rsqrt(jnp.sum(updated * updated, axis=axis, keepdims=True) + EPSILON)
    )


def layout(n, nh, slots, model, width, hidden):
    vmem, dma = pltpu.VMEM, pltpu.SemaphoreType.DMA
    part = PAIR // nh
    rows = part // STEPS
    wide = LANES * (-(-width // LANES))
    tokens = nh * PAIR
    parts = hidden // LANES
    chunk = 8 * (-(-3 * width // (8 * n)))
    outer = n // 2
    sizes = {}
    for c in range(STEPS):
        sizes[f"held{c}"] = vmem((slots, rows, model), BF)
        sizes[f"out{c}"] = vmem((n, rows, model), BF)
        sizes[f"in{c}"] = vmem((n, rows, model), BF)
        sizes[f"chosen{c}"] = vmem((nh, rows, model), BF)
    sizes.update(
        meta=vmem((n, 1, LANES), jnp.int32), meta_in=vmem((n, 1, LANES), jnp.int32),
        codes=pltpu.SMEM((n, 1, LANES), jnp.int32),
        w=vmem((4, nh, width, model), BF),
        pair=vmem((2, STEPS, nh // 2, rows, model), BF),
        q=vmem((PAIR, model), BF), k=vmem((PAIR, model), BF), v=vmem((PAIR, model), BF),
        a=vmem((CHUNK, model), BF), emb=vmem((nh, PAIR, model), BF),
        wf_in=vmem((3, width, model), BF), wr_in=vmem((1, model), BF),
        gu=vmem((2, width, hidden), F32), dt=vmem((width, hidden), F32),
        wf=vmem((3 * wide, model), BF), fq=vmem((tokens, wide), BF), fk=vmem((tokens, wide), BF),
        fkt=vmem((wide, tokens), BF), og=vmem((tokens, wide), BF), ogt=vmem((wide, tokens), BF),
        col=vmem((tokens, width), BF), two=vmem((tokens, 2 * LANES), BF), hk=vmem((tokens, LANES), BF),
        guw=vmem((parts, wide, 2 * LANES), BF), dth=vmem((wide, hidden), BF),
        g=vmem((max(3 * width, chunk * n), LANES), F32),
        total=vmem((max(3 * width, chunk * n), hidden), F32),
        ag=vmem((wide, 2 * hidden), BF), ad=vmem((width, hidden), BF),
        part=vmem((parts, 2, outer, chunk, LANES), BF), xin=vmem((parts, outer, chunk, LANES), BF),
        half=vmem((parts, outer, chunk, LANES), BF), zin=vmem((parts, outer - 1, chunk, LANES), BF),
        res=vmem((parts, 2, outer, chunk, LANES), BF),
        eg_in=vmem((model // LANES, LANES), F32), fg_in=vmem((model // LANES, LANES), F32),
        eg=vmem((1, model), F32), fg=vmem((1, model), F32), done=vmem((tokens, width), BF),
        local=dma((STEPS + 9,)), put=dma((tokens // BLK,)),
        xs=dma((STEPS, n - 1)), xr=dma((STEPS, n - 1)), ms=dma((n - 1,)), mr=dma((n - 1,)),
        ws=dma((3, 4)), wr=dma((3, 4)), ss=dma((STEPS, nh - 1)), sr=dma((STEPS, nh - 1)),
        gs=dma((3, PAIR // CHUNK)), gr=dma((3, PAIR // CHUNK)),
        ps=dma((parts,)), pr=dma((parts,)), zs=dma((parts, outer - 1)), zr=dma((parts, outer - 1)),
        rs=dma((parts, outer)), rr=dma((parts, outer)),
        fs=dma((parts, outer - 1)), fr=dma((parts, outer - 1)),
    )
    return sizes


def gradient_sum(n, width, s, side, lane, compute, during):
    seq = lax.axis_index("seq")
    outer_count = n // 2
    inner, outer = lax.rem(seq, 2), lax.div(seq, 2)
    parts = s.part.shape[0]
    chunk = s.part.shape[3]
    steps = range(1, outer_count)

    def plan(part):
        mine = s.res.at[part, inner, outer]
        theirs = [s.res.at[part, inner, lax.rem(outer + outer_count - t, outer_count)] for t in steps]
        return types.SimpleNamespace(
            x=remote(s.part.at[part, 1 - inner], s.xin.at[part], s.ps.at[part], s.pr.at[part], side),
            z=[
                remote(
                    s.half.at[part, lax.rem(outer + t, outer_count)], s.zin.at[part, t - 1],
                    s.zs.at[part, t - 1], s.zr.at[part, t - 1], lane[t - 1],
                )
                for t in steps
            ],
            r=[
                remote(mine, mine, s.rs.at[part, t], s.rr.at[part, t], to)
                for t, to in enumerate(lane + [side])
            ],
            f=[
                remote(theirs[t - 1], theirs[t - 1], s.fs.at[part, t - 1], s.fr.at[part, t - 1], side)
                for t in steps
            ],
        )

    plans = [plan(part) for part in range(parts)]

    def stage_x(part):
        plans[part].x.start()

    def stage_z(part):
        plans[part].x.wait_recv()
        for o in range(outer_count):
            s.half[part, o] = (
                s.part[part, inner, o].astype(F32) + s.xin[part, o].astype(F32)
            ).astype(BF)
        for copy in plans[part].z:
            copy.start()

    def stage_r(part):
        total = s.half[part, outer].astype(F32)
        for t, copy in enumerate(plans[part].z):
            copy.wait_recv()
            total = total + s.zin[part, t].astype(F32)
        s.res[part, inner, outer] = total.astype(BF)
        for copy in plans[part].r:
            copy.start()

    def stage_f(part):
        for t in steps:
            plans[part].r[t - 1].wait_recv()
            plans[part].f[t - 1].start()

    stages = [stage_x, stage_z, stage_r, stage_f]
    for tick in range(parts + len(stages) - 1):
        if tick < parts:
            compute(tick)
        for which, stage in enumerate(stages):
            if 0 <= tick - which < parts:
                stage(tick - which)
        if tick == parts - 1:
            during()
    for part in range(parts):
        plans[part].r[-1].wait_recv()
        for copy in plans[part].f:
            copy.wait_recv()
        cut = slice(part * LANES, (part + 1) * LANES)
        for i in range(2):
            for o in range(outer_count):
                at = (i * outer_count + o) * chunk
                s.total[at : at + chunk, cut] = s.res[part, i, o].astype(F32)
    for part in range(parts):
        plans[part].x.wait_send()
        for copy in plans[part].z + plans[part].r + plans[part].f:
            copy.wait_send()


def whole_kernel(
    n, nh, names, dest_ref, image_ref, x_ref, wqkv_ref, wo_ref, eg_ref, fg_ref, wf_ref, wr_ref,
    gu_ref, dt_ref, o_ref, *scratch,
):
    s = types.SimpleNamespace(**dict(zip(names, scratch)))
    seq, head = lax.axis_index("seq"), lax.axis_index("head")
    partner = head + 1 - 2 * lax.rem(head, 2)
    peer = lax.rem(head + nh // 2, nh)
    targets = others(n, seq)
    mates = others(nh, head)
    outer_count = n // 2
    inner, outer = lax.rem(seq, 2), lax.div(seq, 2)
    side = (outer * 2 + 1 - inner, head)
    lane = [(lax.rem(outer + t, outer_count) * 2 + inner, head) for t in range(1, outer_count)]
    model = x_ref.shape[-1]
    width, hidden = gu_ref.shape[1:]
    wide = s.fk.shape[1]
    parts = hidden // LANES
    tokens = nh * PAIR
    held = [getattr(s, f"held{c}") for c in range(STEPS)]
    out = [getattr(s, f"out{c}") for c in range(STEPS)]
    arrived = [getattr(s, f"in{c}") for c in range(STEPS)]
    chosen = [getattr(s, f"chosen{c}") for c in range(STEPS)]
    rows = held[0].shape[1]
    per_block = nh // 2

    barrier = pltpu.get_barrier_semaphore()
    greeted = [(to, head) for to in targets] + [(seq, to) for to in mates]
    for device in greeted:
        pl.semaphore_signal(barrier, inc=1, device_id=device, device_id_type=MESH)

    fetch = [
        pltpu.make_async_copy(x_ref.at[:, lax.rem(head, per_block), c], held[c], s.local.at[c])
        for c in range(STEPS)
    ]
    weights_in = [
        pltpu.make_async_copy(wqkv_ref, s.w.at[0:3, head], s.local.at[STEPS]),
        pltpu.make_async_copy(wo_ref, s.w.at[3, head], s.local.at[STEPS + 1]),
    ]
    late = [
        pltpu.make_async_copy(src, dst, s.local.at[STEPS + 2 + which])
        for which, (src, dst) in enumerate(
            [(wf_ref, s.wf_in), (wr_ref, s.wr_in), (gu_ref, s.gu), (dt_ref, s.dt)]
        )
    ]
    gains_in = [
        pltpu.make_async_copy(src, dst, s.local.at[STEPS + 7 + which])
        for which, (src, dst) in enumerate([(eg_ref, s.eg_in), (fg_ref, s.fg_in)])
    ]
    for copy in fetch[:1] + weights_in + fetch[1:] + late + gains_in:
        copy.start()

    my_block = lax.div(head, per_block)
    pairs = dest_ref.shape[0] // 2
    firsts = [dest_ref[2 * i] for i in range(pairs)]
    sames = [(image_ref[2 * i] == image_ref[2 * i + 1]).astype(jnp.int32) for i in range(pairs)]
    homes = [lax.div(jnp.maximum(d, 0), BLK_DEV) for d in firsts]
    slots = []
    for i, d in enumerate(firsts):
        slots.append(2 * i + lax.rem(jnp.maximum(d, 0) + my_block, 2))
    marks = [
        2 * lax.div(lax.rem(jnp.maximum(d, 0), BLK_DEV), 2) + same for d, same in zip(firsts, sames)
    ]

    def lookup(target):
        slot, code = jnp.int32(0), jnp.int32(-1)
        for i, d in enumerate(firsts):
            hit = jnp.logical_and(d >= 0, homes[i] == target)
            slot = jnp.where(hit, slots[i], slot)
            code = jnp.where(hit, marks[i], code)
        return slot, code

    found = [lookup(to) for to in targets + [seq]]
    for step, to in enumerate(targets):
        s.meta[step] = jnp.full((1, LANES), found[step][1], jnp.int32)
    s.meta_in[seq] = jnp.full((1, LANES), found[-1][1], jnp.int32)

    def pick(c):
        fetch[c].wait()
        for step in range(n - 1):
            out[c][step] = held[c][found[step][0]]
        arrived[c][seq] = held[c][found[-1][0]]

    meta_copies = [
        remote(s.meta.at[step], s.meta_in.at[seq], s.ms.at[step], s.mr.at[step], (to, head))
        for step, to in enumerate(targets)
    ]
    x_copies = [
        [
            remote(out[c].at[step], arrived[c].at[seq], s.xs.at[c, step], s.xr.at[c, step], (to, head))
            for step, to in enumerate(targets)
        ]
        for c in range(STEPS)
    ]
    to_peer = [
        remote(s.w.at[m, head], s.w.at[m, head], s.ws.at[0, m], s.wr.at[0, m], (seq, peer))
        for m in range(4)
    ]
    to_partner = [
        remote(s.w.at[m, head], s.w.at[m, head], s.ws.at[1, m], s.wr.at[1, m], (seq, partner))
        for m in range(4)
    ]
    passed = [
        remote(s.w.at[m, peer], s.w.at[m, peer], s.ws.at[2, m], s.wr.at[2, m], (seq, partner))
        for m in range(4)
    ]
    pick(0)
    pl.semaphore_wait(barrier, len(greeted))
    for copy in meta_copies + x_copies[0]:
        copy.start()
    for copy in weights_in:
        copy.wait()
    for copy in to_peer + to_partner:
        copy.start()
    for c in range(1, STEPS):
        pick(c)
        for copy in x_copies[c]:
            copy.start()

    s.wf[...] = jnp.zeros_like(s.wf)
    s.guw[...] = jnp.zeros_like(s.guw)
    s.dth[...] = jnp.zeros_like(s.dth)
    s.g[...] = jnp.zeros_like(s.g)
    s.ag[...] = jnp.zeros_like(s.ag)
    for copy in late + gains_in:
        copy.wait()
    for src, dst in ((s.eg_in, s.eg), (s.fg_in, s.fg)):
        for which in range(model // LANES):
            dst[:, which * LANES : (which + 1) * LANES] = src[which : which + 1]
    for which in range(3):
        s.wf[which * wide : which * wide + width] = s.wf_in[which]
    rate_at = 2 * wide + width
    s.wf[rate_at : rate_at + 16] = jnp.broadcast_to(s.wr_in[...], (16, model))
    s.dth[:width] = s.dt[...].astype(BF)
    for part in range(parts):
        cut = slice(part * LANES, (part + 1) * LANES)
        s.guw[part, :width, :LANES] = s.gu[0, :, cut].astype(BF)
        s.guw[part, :width, LANES:] = s.gu[1, :, cut].astype(BF)

    for copy in meta_copies:
        copy.wait_recv()
    spread = pltpu.make_async_copy(s.meta_in, s.codes, s.local.at[STEPS + 6])
    spread.start()
    spread.wait()
    sources = [jnp.int32(0)] * nh
    same = jnp.int32(0)
    for source in range(n):
        code = s.codes[source, 0, 0]
        place = lax.div(jnp.maximum(code, 0), 2)
        for p in range(nh):
            sources[p] = jnp.where(jnp.logical_and(code >= 0, place == p), source, sources[p])
        mine = jnp.logical_and(code >= 0, place == head)
        same = jnp.where(mine, lax.rem(jnp.maximum(code, 0), 2), same)

    swaps = [
        [
            remote(
                chosen[c].at[to], s.pair.at[lax.div(head, per_block), c, lax.rem(head, per_block)],
                s.ss.at[c, step], s.sr.at[c, step], (seq, to),
            )
            for step, to in enumerate(mates)
        ]
        for c in range(STEPS)
    ]

    def swap(c):
        for copy in x_copies[c]:
            copy.wait_recv()
        for p in range(nh):
            chosen[c][p] = arrived[c][sources[p]]
        for copy in swaps[c]:
            copy.start()
        s.pair[lax.div(head, per_block), c, lax.rem(head, per_block)] = chosen[c][head]

    def matrix(m):
        return s.w[m].reshape(nh * width, model)

    run = per_block * rows

    def project(c):
        for copy in swaps[c]:
            copy.wait_recv()
        taken = jnp.concatenate([s.pair[b, c].reshape(run, model) for b in range(2)], axis=0)
        normed = norm_rows(taken, s.eg[...])
        for m, ref in enumerate((s.q, s.k, s.v)):
            value = dot_nt(normed, matrix(m)).astype(BF)
            if m == 0:
                value = value * BF(HDIM ** (-0.5))
            for b in range(2):
                at = b * BLK + c * run
                ref[at : at + run] = value[b * run : (b + 1) * run]

    def forward(m):
        to_peer[m].wait_recv()
        passed[m].start()

    for c in range(STEPS):
        swap(c)
        if c == STEPS - 2:
            for m in range(4):
                forward(m)
            for m in range(3):
                to_partner[m].wait_recv()
                passed[m].wait_recv()
            for early in range(c):
                project(early)
    project(STEPS - 2)
    project(STEPS - 1)
    to_partner[3].wait_recv()
    passed[3].wait_recv()

    apart = jnp.where(same > 0, 0.0, -1e30).astype(F32)
    key_block = lax.broadcasted_iota(jnp.int32, (1, PAIR), 1) // BLK
    first = lax.broadcasted_iota(jnp.int32, (CHUNK, LANES), 1) < HDIM
    chunks = PAIR // CHUNK

    def emb_copies(i):
        at = pl.ds(i * CHUNK, CHUNK)
        mine, theirs = s.emb.at[head, at], s.emb.at[peer, at]
        return [
            remote(mine, mine, s.gs.at[0, i], s.gr.at[0, i], (seq, peer)),
            remote(mine, mine, s.gs.at[1, i], s.gr.at[1, i], (seq, partner)),
            remote(theirs, theirs, s.gs.at[2, i], s.gr.at[2, i], (seq, partner)),
        ]

    gathers = [emb_copies(i) for i in range(chunks)]

    def attend(i):
        at = pl.ds(i * CHUNK, CHUNK)
        bias = jnp.where(key_block == i * CHUNK // BLK, 0.0, apart)

        def slabs(index, carry):
            for half in range(2):
                columns = pl.ds(pl.multiple_of((2 * index + half) * LANES, LANES), LANES)
                query = s.q[at, columns]
                nothing = jnp.zeros_like(query)
                both = jnp.concatenate(
                    [jnp.where(first, query, nothing), jnp.where(first, nothing, query)], axis=0
                )
                scores = dot_nt(both, s.k[:, columns]) + bias
                top = jnp.max(scores, axis=-1, keepdims=True)
                weights = jnp.exp(scores - top)
                total = jnp.sum(weights, axis=-1, keepdims=True)
                mixed = dot(weights.astype(BF), s.v[:, columns]) * (1.0 / total)
                s.a[:, columns] = jnp.where(first, mixed[:CHUNK], mixed[CHUNK:]).astype(BF)
            return carry

        lax.fori_loop(0, model // LANES // 2, slabs, 0)
        mixed = dot(s.a[...], matrix(3))
        taken = s.pair[i * CHUNK // BLK].reshape(BLK, model)
        low = i * CHUNK % BLK
        s.emb[head, at] = (taken[low : low + CHUNK].astype(F32) + mixed).astype(BF)
        gathers[i][0].start()
        gathers[i][1].start()

    scale = RATE_SCALE * (tokens * n) ** (-0.5)

    def fast_project(owner, i):
        at = pl.ds(pl.multiple_of(owner * PAIR + i * CHUNK, CHUNK), CHUNK)
        normed = norm_rows(s.emb[owner, pl.ds(i * CHUNK, CHUNK)], s.fg[...])
        mapped = dot_nt(normed, s.wf[...])
        s.fq[at] = mapped[:, :wide].astype(BF)
        key = mapped[:, wide : 2 * wide].astype(BF)
        s.fk[at] = key
        s.fkt[:, at] = key.T
        value = mapped[:, 2 * wide :].astype(BF).astype(F32)
        before = mapped[:, rate_at : rate_at + 1]
        soft = jnp.maximum(before, 0.0) + jnp.log1p(jnp.exp(-jnp.abs(before)))
        back = (-(scale * soft) * value).astype(BF)
        s.og[at] = back
        s.ogt[:, at] = back.T

    for i in range(chunks):
        attend(i)
        fast_project(head, i)
        if i >= 1:
            gathers[i - 1][0].wait_recv()
            gathers[i - 1][2].start()
    across = lax.rem(partner + nh // 2, nh)
    for i in range(chunks - 1):
        gathers[i][1].wait_recv()
        fast_project(partner, i)
        fast_project(peer, i)
    gathers[chunks - 1][1].wait_recv()
    fast_project(partner, chunks - 1)
    for i in range(chunks - 1):
        gathers[i][2].wait_recv()
        fast_project(across, i)
    gathers[chunks - 1][0].wait_recv()
    gathers[chunks - 1][2].start()
    fast_project(peer, chunks - 1)
    gathers[chunks - 1][2].wait_recv()
    fast_project(across, chunks - 1)

    def compute(part):
        def body(unit, carry):
            at = pl.ds(pl.multiple_of(unit * UNIT, UNIT), UNIT)
            both = dot(s.fk[at], s.guw[part])
            gate, up = both[:, :LANES], both[:, LANES:]
            grad = dot(s.og[at], s.dth[:, part * LANES : (part + 1) * LANES])
            sig = jax.nn.sigmoid(gate)
            silu = gate * sig
            s.hk[at] = (silu * up).astype(BF)
            s.two[at, :LANES] = (grad * up * sig * (1.0 + gate * (1.0 - sig))).astype(BF)
            s.two[at, LANES:] = (grad * silu).astype(BF)
            return carry

        lax.fori_loop(0, tokens // UNIT, body, 0, unroll=2)
        one = dot(s.fkt[...], s.two[...])
        other = dot(s.ogt[...], s.hk[...])
        s.g[0:width] = one[:width, :LANES]
        s.g[width : 2 * width] = one[:width, LANES:]
        s.g[2 * width : 3 * width] = other[:width]
        chunk = s.part.shape[3]
        for i in range(2):
            for o in range(outer_count):
                at = (i * outer_count + o) * chunk
                s.part[part, i, o] = s.g[at : at + chunk].astype(BF)

    def during():
        for which in range(model // width):

            @pl.when(head == which)
            def _():
                for owner in range(nh):
                    at = owner * PAIR
                    s.col[at : at + PAIR] = s.emb[owner, :, which * width : (which + 1) * width]

    gradient_sum(n, width, s, side, lane, compute, during)

    for which in range(2):
        start = s.gu[which]
        fresh = renorm(start - s.total[which * width : (which + 1) * width], start, 1)
        s.ag[:width, which * hidden : (which + 1) * hidden] = fresh.astype(BF)
    start = s.dt[...]
    s.ad[...] = renorm(start - s.total[2 * width : 3 * width], start, 0).astype(BF)

    def put(unit):
        at = pl.ds(unit * BLK, BLK)
        return pltpu.make_async_copy(s.done.at[at], o_ref.at[at], s.put.at[unit])

    def final(unit, carry):
        base = pl.multiple_of(unit * BLK, BLK)
        at = pl.ds(base, BLK)
        both = dot(s.fq[at], s.ag[...])
        gate = both[:, :hidden]
        inside = (gate * jax.nn.sigmoid(gate) * both[:, hidden:]).astype(BF)
        done = (s.col[at].astype(F32) + dot_nt(inside, s.ad[...])).astype(BF)
        for c in range(STEPS):
            for which in range(per_block):
                low = (c * per_block + which) * rows
                to = pl.multiple_of(base + which * STEPS * rows + c * rows, rows)
                s.done[pl.ds(to, rows)] = done[low : low + rows]
        put(unit).start()
        return carry

    lax.fori_loop(0, tokens // BLK, final, 0, unroll=2)
    for unit in range(tokens // BLK):
        put(unit).wait()

    for copy in meta_copies + to_peer + to_partner + passed:
        copy.wait_send()
    for group in x_copies + swaps + gathers:
        for copy in group:
            copy.wait_send()


def on_device(
    patches,
    slot_image,
    slot_dest,
    enc_gain,
    w_qkv,
    w_out,
    fast_gain,
    w_fast,
    w_rate,
    fast_gate_up,
    fast_down,
):
    n = lax.axis_size("seq")
    nh = lax.axis_size("head")
    model = patches.shape[1]
    slots = slot_dest.shape[0]
    width, hidden = fast_gate_up.shape[2:]
    part = PAIR // nh
    sizes = layout(n, nh, slots, model, width, hidden)
    return pl.pallas_call(
        functools.partial(whole_kernel, n, nh, tuple(sizes)),
        out_shape=jax.ShapeDtypeStruct((nh * PAIR, width), patches.dtype),
        in_specs=[SMEM, SMEM] + [ANY] * 9,
        out_specs=ANY,
        scratch_shapes=list(sizes.values()),
        compiler_params=pltpu.CompilerParams(
            collective_id=1, has_side_effects=True, vmem_limit_bytes=60 * 1024 * 1024
        ),
        name="encode_and_update",
    )(
        slot_dest,
        slot_image,
        patches.reshape(slots, BLK // part, STEPS, part // STEPS, model),
        jnp.swapaxes(w_qkv, 1, 2),
        w_out,
        enc_gain.reshape(model // LANES, LANES),
        fast_gain.reshape(model // LANES, LANES),
        jnp.swapaxes(w_fast, 1, 2),
        w_rate.T,
        fast_gate_up[0],
        fast_down[0].T,
    )


def solution(mesh):
    in_specs = (
        P("seq", None),
        P("seq"),
        P("seq"),
        P(),
        P(None, None, "head"),
        P("head", None),
        P(),
        P(None, None, "head"),
        P(None, "head"),
        P("head", None, None, None),
        P("head", None, None),
    )
    out_specs = P("seq", "head")
    return jax.shard_map(
        on_device, mesh=mesh, in_specs=in_specs, out_specs=out_specs, check_vma=False
    )
```

```python
import functools
import types

import jax
import jax.numpy as jnp
from jax import lax
from jax.experimental import pallas as pl
from jax.experimental.pallas import tpu as pltpu
from jax.sharding import PartitionSpec as P

HDIM = 64
BLK = 256
BLK_DEV = 8
PAIR = 2 * BLK
EPSILON = 1e-06
RATE_SCALE = 0.1
LANES = 128
STEPS = 4
CHUNK = 128
UNIT = 256
MESH = pl.DeviceIdType.MESH
VMEM = pl.BlockSpec(memory_space=pltpu.VMEM)
SMEM = pl.BlockSpec(memory_space=pltpu.SMEM)
ANY = pl.BlockSpec(memory_space=pl.ANY)
NT = (((1,), (1,)), ((), ()))
BF = jnp.bfloat16
F32 = jnp.float32


def remote(src, dst, send, recv, device):
    return pltpu.make_async_remote_copy(
        src_ref=src, dst_ref=dst, send_sem=send, recv_sem=recv, device_id=device, device_id_type=MESH
    )


def others(axis_size, me):
    return [lax.rem(me + step, axis_size) for step in range(1, axis_size)]


def dot(a, b):
    return jnp.dot(a, b, preferred_element_type=F32)


def dot_nt(a, b):
    return lax.dot_general(a, b, NT, preferred_element_type=F32)


def norm_rows(values, gain):
    wide = values.astype(F32)
    factor = lax.rsqrt(jnp.mean(wide * wide, axis=-1, keepdims=True) + EPSILON)
    return (wide * factor * gain).astype(BF)


def renorm(updated, initial, axis):
    target_norm = jnp.sqrt(jnp.sum(initial * initial, axis=axis, keepdims=True))
    return (
        updated
        * target_norm
        * lax.rsqrt(jnp.sum(updated * updated, axis=axis, keepdims=True) + EPSILON)
    )


def layout(n, nh, slots, model, width, hidden):
    vmem, dma = pltpu.VMEM, pltpu.SemaphoreType.DMA
    part = PAIR // nh
    rows = part // STEPS
    wide = LANES * (-(-width // LANES))
    tokens = nh * PAIR
    parts = hidden // LANES
    chunk = 8 * (-(-3 * width // (8 * n)))
    outer = n // 2
    sizes = {}
    for c in range(STEPS):
        sizes[f"held{c}"] = vmem((slots, rows, model), BF)
        sizes[f"out{c}"] = vmem((n, rows, model), BF)
        sizes[f"in{c}"] = vmem((n, rows, model), BF)
        sizes[f"chosen{c}"] = vmem((nh, rows, model), BF)
    sizes.update(
        meta=vmem((n, 1, LANES), jnp.int32), meta_in=vmem((n, 1, LANES), jnp.int32),
        codes=pltpu.SMEM((n, 1, LANES), jnp.int32),
        w=vmem((4, nh, width, model), BF),
        pair=vmem((2, STEPS, nh // 2, rows, model), BF),
        q=vmem((PAIR, model), BF), k=vmem((PAIR, model), BF), v=vmem((PAIR, 2 * model), BF),
        a=vmem((CHUNK, model), BF), emb=vmem((nh, PAIR, model), BF),
        wf_in=vmem((3, width, model), BF), wr_in=vmem((1, model), BF),
        gu=vmem((2, width, hidden), F32), dt=vmem((width, hidden), F32),
        wf=vmem((3 * wide, model), BF), fq=vmem((tokens, wide), BF),
        fkt=vmem((wide, tokens), BF), ogt=vmem((wide, tokens), BF),
        col=vmem((tokens, width), BF), two=vmem((parts, tokens, 2 * LANES), BF),
        hk=vmem((parts, tokens, LANES), BF),
        guw=vmem((parts, wide, 2 * LANES), BF), dth=vmem((wide, hidden), BF),
        g=vmem((max(3 * width, chunk * n), LANES), F32),
        total=vmem((max(3 * width, chunk * n), hidden), F32),
        ag=vmem((wide, 2 * hidden), BF), ad=vmem((width, hidden), BF),
        part=vmem((parts, 2, outer, chunk, LANES), BF), xin=vmem((parts, outer, chunk, LANES), BF),
        half=vmem((parts, outer, chunk, LANES), BF), zin=vmem((parts, outer - 1, chunk, LANES), BF),
        res=vmem((parts, 2, outer, chunk, LANES), BF),
        eg_in=vmem((model // LANES, LANES), F32), fg_in=vmem((model // LANES, LANES), F32),
        eg=vmem((1, model), F32), fg=vmem((1, model), F32), done=vmem((tokens, width), BF),
        local=dma((STEPS + 9,)), put=dma((tokens // BLK,)),
        xs=dma((STEPS, n - 1)), xr=dma((STEPS, n - 1)), ms=dma((n - 1,)), mr=dma((n - 1,)),
        ws=dma((3, 4)), wr=dma((3, 4)), ss=dma((STEPS, nh - 1)), sr=dma((STEPS, nh - 1)),
        gs=dma((3, PAIR // CHUNK)), gr=dma((3, PAIR // CHUNK)),
        ps=dma((parts,)), pr=dma((parts,)), zs=dma((parts, outer - 1)), zr=dma((parts, outer - 1)),
        rs=dma((parts, outer)), rr=dma((parts, outer)),
        fs=dma((parts, outer - 1)), fr=dma((parts, outer - 1)),
    )
    return sizes


def gradient_sum(n, width, s, side, lane, compute, during):
    seq = lax.axis_index("seq")
    outer_count = n // 2
    inner, outer = lax.rem(seq, 2), lax.div(seq, 2)
    parts = s.part.shape[0]
    chunk = s.part.shape[3]
    steps = range(1, outer_count)

    def plan(part):
        mine = s.res.at[part, inner, outer]
        theirs = [s.res.at[part, inner, lax.rem(outer + outer_count - t, outer_count)] for t in steps]
        return types.SimpleNamespace(
            x=remote(s.part.at[part, 1 - inner], s.xin.at[part], s.ps.at[part], s.pr.at[part], side),
            z=[
                remote(
                    s.half.at[part, lax.rem(outer + t, outer_count)], s.zin.at[part, t - 1],
                    s.zs.at[part, t - 1], s.zr.at[part, t - 1], lane[t - 1],
                )
                for t in steps
            ],
            r=[
                remote(mine, mine, s.rs.at[part, t], s.rr.at[part, t], to)
                for t, to in enumerate(lane + [side])
            ],
            f=[
                remote(theirs[t - 1], theirs[t - 1], s.fs.at[part, t - 1], s.fr.at[part, t - 1], side)
                for t in steps
            ],
        )

    plans = [plan(part) for part in range(parts)]

    def stage_x(part):
        plans[part].x.start()

    def stage_z(part):
        plans[part].x.wait_recv()
        for o in range(outer_count):
            s.half[part, o] = (
                s.part[part, inner, o].astype(F32) + s.xin[part, o].astype(F32)
            ).astype(BF)
        for copy in plans[part].z:
            copy.start()

    def stage_r(part):
        total = s.half[part, outer].astype(F32)
        for t, copy in enumerate(plans[part].z):
            copy.wait_recv()
            total = total + s.zin[part, t].astype(F32)
        s.res[part, inner, outer] = total.astype(BF)
        for copy in plans[part].r:
            copy.start()

    def stage_f(part):
        for t in steps:
            plans[part].r[t - 1].wait_recv()
            plans[part].f[t - 1].start()

    stages = [stage_x, stage_z, stage_r, stage_f]
    for tick in range(parts + len(stages) - 1):
        if tick < parts:
            compute(tick)
        for which, stage in enumerate(stages):
            if 0 <= tick - which < parts:
                stage(tick - which)
        if tick == parts - 1:
            during()
    for part in range(parts):
        plans[part].r[-1].wait_recv()
        for copy in plans[part].f:
            copy.wait_recv()
        cut = slice(part * LANES, (part + 1) * LANES)
        for i in range(2):
            for o in range(outer_count):
                at = (i * outer_count + o) * chunk
                s.total[at : at + chunk, cut] = s.res[part, i, o].astype(F32)
    for part in range(parts):
        plans[part].x.wait_send()
        for copy in plans[part].z + plans[part].r + plans[part].f:
            copy.wait_send()


def whole_kernel(
    n, nh, names, dest_ref, image_ref, x_ref, wqkv_ref, wo_ref, eg_ref, fg_ref, wf_ref, wr_ref,
    gu_ref, dt_ref, o_ref, *scratch,
):
    s = types.SimpleNamespace(**dict(zip(names, scratch)))
    seq, head = lax.axis_index("seq"), lax.axis_index("head")
    partner = head + 1 - 2 * lax.rem(head, 2)
    peer = lax.rem(head + nh // 2, nh)
    targets = others(n, seq)
    mates = others(nh, head)
    outer_count = n // 2
    inner, outer = lax.rem(seq, 2), lax.div(seq, 2)
    side = (outer * 2 + 1 - inner, head)
    lane = [(lax.rem(outer + t, outer_count) * 2 + inner, head) for t in range(1, outer_count)]
    model = x_ref.shape[-1]
    width, hidden = gu_ref.shape[1:]
    wide = s.fq.shape[1]
    parts = hidden // LANES
    tokens = nh * PAIR
    held = [getattr(s, f"held{c}") for c in range(STEPS)]
    out = [getattr(s, f"out{c}") for c in range(STEPS)]
    arrived = [getattr(s, f"in{c}") for c in range(STEPS)]
    chosen = [getattr(s, f"chosen{c}") for c in range(STEPS)]
    rows = held[0].shape[1]
    per_block = nh // 2

    barrier = pltpu.get_barrier_semaphore()
    greeted = [(to, head) for to in targets] + [(seq, to) for to in mates]
    for device in greeted:
        pl.semaphore_signal(barrier, inc=1, device_id=device, device_id_type=MESH)

    fetch = [
        pltpu.make_async_copy(x_ref.at[:, lax.rem(head, per_block), c], held[c], s.local.at[c])
        for c in range(STEPS)
    ]
    weights_in = [
        pltpu.make_async_copy(wqkv_ref, s.w.at[0:3, head], s.local.at[STEPS]),
        pltpu.make_async_copy(wo_ref, s.w.at[3, head], s.local.at[STEPS + 1]),
    ]
    late = [
        pltpu.make_async_copy(src, dst, s.local.at[STEPS + 2 + which])
        for which, (src, dst) in enumerate(
            [(wf_ref, s.wf_in), (wr_ref, s.wr_in), (gu_ref, s.gu), (dt_ref, s.dt)]
        )
    ]
    gains_in = [
        pltpu.make_async_copy(src, dst, s.local.at[STEPS + 7 + which])
        for which, (src, dst) in enumerate([(eg_ref, s.eg_in), (fg_ref, s.fg_in)])
    ]
    for copy in fetch[:1] + weights_in + fetch[1:] + late + gains_in:
        copy.start()

    my_block = lax.div(head, per_block)
    pairs = dest_ref.shape[0] // 2
    firsts = [dest_ref[2 * i] for i in range(pairs)]
    sames = [(image_ref[2 * i] == image_ref[2 * i + 1]).astype(jnp.int32) for i in range(pairs)]
    homes = [lax.div(jnp.maximum(d, 0), BLK_DEV) for d in firsts]
    slots = []
    for i, d in enumerate(firsts):
        slots.append(2 * i + lax.rem(jnp.maximum(d, 0) + my_block, 2))
    marks = [
        2 * lax.div(lax.rem(jnp.maximum(d, 0), BLK_DEV), 2) + same for d, same in zip(firsts, sames)
    ]

    def lookup(target):
        slot, code = jnp.int32(0), jnp.int32(-1)
        for i, d in enumerate(firsts):
            hit = jnp.logical_and(d >= 0, homes[i] == target)
            slot = jnp.where(hit, slots[i], slot)
            code = jnp.where(hit, marks[i], code)
        return slot, code

    found = [lookup(to) for to in targets + [seq]]
    for step, to in enumerate(targets):
        s.meta[step] = jnp.full((1, LANES), found[step][1], jnp.int32)
    s.meta_in[seq] = jnp.full((1, LANES), found[-1][1], jnp.int32)

    def pick(c):
        fetch[c].wait()
        for step in range(n - 1):
            out[c][step] = held[c][found[step][0]]
        arrived[c][seq] = held[c][found[-1][0]]

    meta_copies = [
        remote(s.meta.at[step], s.meta_in.at[seq], s.ms.at[step], s.mr.at[step], (to, head))
        for step, to in enumerate(targets)
    ]
    x_copies = [
        [
            remote(out[c].at[step], arrived[c].at[seq], s.xs.at[c, step], s.xr.at[c, step], (to, head))
            for step, to in enumerate(targets)
        ]
        for c in range(STEPS)
    ]
    to_peer = [
        remote(s.w.at[m, head], s.w.at[m, head], s.ws.at[0, m], s.wr.at[0, m], (seq, peer))
        for m in range(4)
    ]
    to_partner = [
        remote(s.w.at[m, head], s.w.at[m, head], s.ws.at[1, m], s.wr.at[1, m], (seq, partner))
        for m in range(4)
    ]
    passed = [
        remote(s.w.at[m, peer], s.w.at[m, peer], s.ws.at[2, m], s.wr.at[2, m], (seq, partner))
        for m in range(4)
    ]
    pick(0)
    pl.semaphore_wait(barrier, len(greeted))
    for copy in meta_copies + x_copies[0]:
        copy.start()
    for copy in weights_in:
        copy.wait()
    for copy in to_peer + to_partner:
        copy.start()
    for c in range(1, STEPS):
        pick(c)
        for copy in x_copies[c]:
            copy.start()

    s.wf[...] = jnp.zeros_like(s.wf)
    s.v[...] = jnp.ones_like(s.v)
    s.guw[...] = jnp.zeros_like(s.guw)
    s.dth[...] = jnp.zeros_like(s.dth)
    s.g[...] = jnp.zeros_like(s.g)
    s.ag[...] = jnp.zeros_like(s.ag)
    for copy in late + gains_in:
        copy.wait()
    for src, dst in ((s.eg_in, s.eg), (s.fg_in, s.fg)):
        for which in range(model // LANES):
            dst[:, which * LANES : (which + 1) * LANES] = src[which : which + 1]
    for which in range(3):
        s.wf[which * wide : which * wide + width] = s.wf_in[which]
    rate_at = 2 * wide + width
    s.wf[rate_at : rate_at + 16] = jnp.broadcast_to(s.wr_in[...], (16, model))
    s.dth[:width] = s.dt[...].astype(BF)
    for part in range(parts):
        cut = slice(part * LANES, (part + 1) * LANES)
        s.guw[part, :width, :LANES] = s.gu[0, :, cut].astype(BF)
        s.guw[part, :width, LANES:] = s.gu[1, :, cut].astype(BF)

    for copy in meta_copies:
        copy.wait_recv()
    spread = pltpu.make_async_copy(s.meta_in, s.codes, s.local.at[STEPS + 6])
    spread.start()
    spread.wait()
    sources = [jnp.int32(0)] * nh
    same = jnp.int32(0)
    for source in range(n):
        code = s.codes[source, 0, 0]
        place = lax.div(jnp.maximum(code, 0), 2)
        for p in range(nh):
            sources[p] = jnp.where(jnp.logical_and(code >= 0, place == p), source, sources[p])
        mine = jnp.logical_and(code >= 0, place == head)
        same = jnp.where(mine, lax.rem(jnp.maximum(code, 0), 2), same)

    swaps = [
        [
            remote(
                chosen[c].at[to], s.pair.at[lax.div(head, per_block), c, lax.rem(head, per_block)],
                s.ss.at[c, step], s.sr.at[c, step], (seq, to),
            )
            for step, to in enumerate(mates)
        ]
        for c in range(STEPS)
    ]

    def swap(c):
        for copy in x_copies[c]:
            copy.wait_recv()
        for p in range(nh):
            chosen[c][p] = arrived[c][sources[p]]
        for copy in swaps[c]:
            copy.start()
        s.pair[lax.div(head, per_block), c, lax.rem(head, per_block)] = chosen[c][head]

    def matrix(m):
        return s.w[m].reshape(nh * width, model)

    run = per_block * rows

    def project(c):
        for copy in swaps[c]:
            copy.wait_recv()
        taken = jnp.concatenate([s.pair[b, c].reshape(run, model) for b in range(2)], axis=0)
        normed = norm_rows(taken, s.eg[...])
        values = [dot_nt(normed, matrix(m)).astype(BF) for m in range(3)]
        values[0] = values[0] * BF(HDIM ** (-0.5))
        for b in range(2):
            at = b * BLK + c * run
            s.q[at : at + run] = values[0][b * run : (b + 1) * run]
            s.k[at : at + run] = values[1][b * run : (b + 1) * run]
            for slab in range(model // LANES):
                s.v[at : at + run, 2 * slab * LANES : (2 * slab + 1) * LANES] = values[2][
                    b * run : (b + 1) * run, slab * LANES : (slab + 1) * LANES
                ]

    def forward(m):
        to_peer[m].wait_recv()
        passed[m].start()

    for c in range(STEPS):
        swap(c)
        if c == STEPS - 2:
            for m in range(4):
                forward(m)
            for m in range(3):
                to_partner[m].wait_recv()
                passed[m].wait_recv()
            for early in range(c):
                project(early)
    project(STEPS - 2)
    project(STEPS - 1)
    to_partner[3].wait_recv()
    passed[3].wait_recv()

    apart = jnp.where(same > 0, 0.0, -1e30).astype(F32)
    key_block = lax.broadcasted_iota(jnp.int32, (1, PAIR), 1) // BLK
    first = lax.broadcasted_iota(jnp.int32, (CHUNK, LANES), 1) < HDIM
    chunks = PAIR // CHUNK

    def emb_copies(i):
        at = pl.ds(pl.multiple_of(i * CHUNK, CHUNK), CHUNK)
        mine, theirs = s.emb.at[head, at], s.emb.at[peer, at]
        return types.SimpleNamespace(
            peer=remote(mine, mine, s.gs.at[0, i], s.gr.at[0, i], (seq, peer)),
            partner=remote(mine, mine, s.gs.at[1, i], s.gr.at[1, i], (seq, partner)),
            across=remote(theirs, theirs, s.gs.at[2, i], s.gr.at[2, i], (seq, partner)),
        )

    per_chunk = CHUNK // run

    def attend(i):
        at = pl.ds(pl.multiple_of(i * CHUNK, CHUNK), CHUNK)
        block = lax.div(i, BLK // CHUNK)
        bias = jnp.where(key_block == block, 0.0, apart)
        for slab in range(model // LANES):
            columns = slice(slab * LANES, (slab + 1) * LANES)
            query = s.q[at, columns]
            nothing = jnp.zeros_like(query)
            both = jnp.concatenate(
                [jnp.where(first, query, nothing), jnp.where(first, nothing, query)], axis=0
            )
            scores = dot_nt(both, s.k[:, columns]) + bias
            top = jnp.max(scores, axis=-1, keepdims=True)
            weights = jnp.exp(scores - top).astype(BF)
            mixed = dot(weights, s.v[:, 2 * slab * LANES : 2 * (slab + 1) * LANES])
            mixed = mixed[:, :LANES] * (1.0 / mixed[:, LANES:])
            s.a[:, columns] = jnp.where(first, mixed[:CHUNK], mixed[CHUNK:]).astype(BF)
        mixed = dot(s.a[...], matrix(3))
        low = lax.rem(i, BLK // CHUNK) * per_chunk
        taken = s.pair[block, pl.ds(low, per_chunk)].reshape(CHUNK, model)
        s.emb[head, at] = (taken.astype(F32) + mixed).astype(BF)

    scale = RATE_SCALE * (tokens * n) ** (-0.5)

    def fast_project(owner, i):
        at = pl.ds(pl.multiple_of(owner * PAIR + i * CHUNK, CHUNK), CHUNK)
        normed = norm_rows(s.emb[owner, pl.ds(i * CHUNK, CHUNK)], s.fg[...])
        mapped = dot_nt(normed, s.wf[...])
        s.fq[at] = mapped[:, :wide].astype(BF)
        key = mapped[:, wide : 2 * wide].astype(BF)
        s.fkt[:, at] = key.T
        value = mapped[:, 2 * wide :].astype(BF).astype(F32)
        before = mapped[:, rate_at : rate_at + 1]
        soft = jnp.maximum(before, 0.0) + jnp.log1p(jnp.exp(-jnp.abs(before)))
        back = (-(scale * soft) * value).astype(BF)
        s.ogt[:, at] = back.T
        for part in range(parts):
            both = dot(key, s.guw[part])
            gate, up = both[:, :LANES], both[:, LANES:]
            grad = dot(back, s.dth[:, part * LANES : (part + 1) * LANES])
            sig = jax.nn.sigmoid(gate)
            silu = gate * sig
            s.hk[part, at] = (silu * up).astype(BF)
            s.two[part, at, :LANES] = (grad * up * sig * (1.0 + gate * (1.0 - sig))).astype(BF)
            s.two[part, at, LANES:] = (grad * silu).astype(BF)

    def own_chunk(i, carry):
        attend(i)
        copies = emb_copies(i)
        copies.peer.start()
        copies.partner.start()
        fast_project(head, i)

        @pl.when(i >= 1)
        def _():
            before = emb_copies(i - 1)
            before.peer.wait_recv()
            before.across.start()

        return carry

    lax.fori_loop(0, chunks, own_chunk, 0)
    across = lax.rem(partner + nh // 2, nh)

    def other_chunk(step, carry):
        i, which = lax.div(step, 3), lax.rem(step, 3)
        copies = emb_copies(i)

        @pl.when(which == 0)
        def _():
            copies.partner.wait_recv()

        @pl.when(jnp.logical_and(which == 1, i == chunks - 1))
        def _():
            copies.peer.wait_recv()
            copies.across.start()

        @pl.when(which == 2)
        def _():
            copies.across.wait_recv()

        fast_project(jnp.where(which == 0, partner, jnp.where(which == 1, peer, across)), i)
        return carry

    lax.fori_loop(0, 3 * chunks, other_chunk, 0)

    def compute(part):
        one = dot(s.fkt[...], s.two[part])
        other = dot(s.ogt[...], s.hk[part])
        s.g[0:width] = one[:width, :LANES]
        s.g[width : 2 * width] = one[:width, LANES:]
        s.g[2 * width : 3 * width] = other[:width]
        chunk = s.part.shape[3]
        for i in range(2):
            for o in range(outer_count):
                at = (i * outer_count + o) * chunk
                s.part[part, i, o] = s.g[at : at + chunk].astype(BF)

    def during():
        for which in range(model // width):

            @pl.when(head == which)
            def _():
                for owner in range(nh):
                    at = owner * PAIR
                    s.col[at : at + PAIR] = s.emb[owner, :, which * width : (which + 1) * width]

    gradient_sum(n, width, s, side, lane, compute, during)

    for which in range(2):
        start = s.gu[which]
        fresh = renorm(start - s.total[which * width : (which + 1) * width], start, 1)
        s.ag[:width, which * hidden : (which + 1) * hidden] = fresh.astype(BF)
    start = s.dt[...]
    s.ad[...] = renorm(start - s.total[2 * width : 3 * width], start, 0).astype(BF)

    def put(unit):
        at = pl.ds(unit * BLK, BLK)
        return pltpu.make_async_copy(s.done.at[at], o_ref.at[at], s.put.at[unit])

    def final(unit, carry):
        base = pl.multiple_of(unit * BLK, BLK)
        at = pl.ds(base, BLK)
        both = dot(s.fq[at], s.ag[...])
        gate = both[:, :hidden]
        inside = (gate * jax.nn.sigmoid(gate) * both[:, hidden:]).astype(BF)
        done = (s.col[at].astype(F32) + dot_nt(inside, s.ad[...])).astype(BF)
        for c in range(STEPS):
            for which in range(per_block):
                low = (c * per_block + which) * rows
                to = pl.multiple_of(base + which * STEPS * rows + c * rows, rows)
                s.done[pl.ds(to, rows)] = done[low : low + rows]
        put(unit).start()
        return carry

    lax.fori_loop(0, tokens // BLK, final, 0, unroll=2)
    for unit in range(tokens // BLK):
        put(unit).wait()

    for copy in meta_copies + to_peer + to_partner + passed:
        copy.wait_send()
    for group in x_copies + swaps:
        for copy in group:
            copy.wait_send()
    for i in range(chunks):
        copies = emb_copies(i)
        for copy in (copies.peer, copies.partner, copies.across):
            copy.wait_send()


def on_device(
    patches,
    slot_image,
    slot_dest,
    enc_gain,
    w_qkv,
    w_out,
    fast_gain,
    w_fast,
    w_rate,
    fast_gate_up,
    fast_down,
):
    n = lax.axis_size("seq")
    nh = lax.axis_size("head")
    model = patches.shape[1]
    slots = slot_dest.shape[0]
    width, hidden = fast_gate_up.shape[2:]
    part = PAIR // nh
    sizes = layout(n, nh, slots, model, width, hidden)
    return pl.pallas_call(
        functools.partial(whole_kernel, n, nh, tuple(sizes)),
        out_shape=jax.ShapeDtypeStruct((nh * PAIR, width), patches.dtype),
        in_specs=[SMEM, SMEM] + [ANY] * 9,
        out_specs=ANY,
        scratch_shapes=list(sizes.values()),
        compiler_params=pltpu.CompilerParams(
            collective_id=1, has_side_effects=True, vmem_limit_bytes=60 * 1024 * 1024
        ),
        name="encode_and_update",
    )(
        slot_dest,
        slot_image,
        patches.reshape(slots, BLK // part, STEPS, part // STEPS, model),
        jnp.swapaxes(w_qkv, 1, 2),
        w_out,
        enc_gain.reshape(model // LANES, LANES),
        fast_gain.reshape(model // LANES, LANES),
        jnp.swapaxes(w_fast, 1, 2),
        w_rate.T,
        fast_gate_up[0],
        fast_down[0].T,
    )


def solution(mesh):
    in_specs = (
        P("seq", None),
        P("seq"),
        P("seq"),
        P(),
        P(None, None, "head"),
        P("head", None),
        P(),
        P(None, None, "head"),
        P(None, "head"),
        P("head", None, None, None),
        P("head", None, None),
    )
    out_specs = P("seq", "head")
    return jax.shard_map(
        on_device, mesh=mesh, in_specs=in_specs, out_specs=out_specs, check_vma=False
    )
```

```python
import functools
import types

import jax
import jax.numpy as jnp
from jax import lax
from jax.experimental import pallas as pl
from jax.experimental.pallas import tpu as pltpu
from jax.sharding import PartitionSpec as P

HDIM = 64
BLK = 256
BLK_DEV = 8
PAIR = 2 * BLK
EPSILON = 1e-06
RATE_SCALE = 0.1
LANES = 128
STEPS = 4
CHUNK = 128
UNIT = 256
MESH = pl.DeviceIdType.MESH
VMEM = pl.BlockSpec(memory_space=pltpu.VMEM)
SMEM = pl.BlockSpec(memory_space=pltpu.SMEM)
ANY = pl.BlockSpec(memory_space=pl.ANY)
NT = (((1,), (1,)), ((), ()))
BF = jnp.bfloat16
F32 = jnp.float32


def remote(src, dst, send, recv, device):
    return pltpu.make_async_remote_copy(
        src_ref=src, dst_ref=dst, send_sem=send, recv_sem=recv, device_id=device, device_id_type=MESH
    )


def others(axis_size, me):
    return [lax.rem(me + step, axis_size) for step in range(1, axis_size)]


def dot(a, b):
    return jnp.dot(a, b, preferred_element_type=F32)


def dot_nt(a, b):
    return lax.dot_general(a, b, NT, preferred_element_type=F32)


def norm_rows(values, gain):
    wide = values.astype(F32)
    factor = lax.rsqrt(jnp.mean(wide * wide, axis=-1, keepdims=True) + EPSILON)
    return (wide * factor * gain).astype(BF)


def renorm(updated, initial, axis):
    target_norm = jnp.sqrt(jnp.sum(initial * initial, axis=axis, keepdims=True))
    return (
        updated
        * target_norm
        * lax.rsqrt(jnp.sum(updated * updated, axis=axis, keepdims=True) + EPSILON)
    )


def layout(n, nh, slots, model, width, hidden):
    vmem, dma = pltpu.VMEM, pltpu.SemaphoreType.DMA
    part = PAIR // nh
    rows = part // STEPS
    wide = LANES * (-(-width // LANES))
    tokens = nh * PAIR
    parts = hidden // LANES
    chunk = 8 * (-(-3 * width // (8 * n)))
    outer = n // 2
    sizes = {}
    for c in range(STEPS):
        sizes[f"held{c}"] = vmem((slots, rows, model), BF)
        sizes[f"out{c}"] = vmem((n, rows, model), BF)
        sizes[f"in{c}"] = vmem((n, rows, model), BF)
        sizes[f"chosen{c}"] = vmem((nh, rows, model), BF)
    sizes.update(
        meta=vmem((n, 1, LANES), jnp.int32), meta_in=vmem((n, 1, LANES), jnp.int32),
        codes=pltpu.SMEM((n, 1, LANES), jnp.int32),
        w=vmem((4, nh, width, model), BF),
        pair=vmem((2, STEPS, nh // 2, rows, model), BF),
        q=vmem((PAIR, model), BF), k=vmem((PAIR, model), BF), v=vmem((PAIR, 2 * model), BF),
        a=vmem((CHUNK, model), BF), emb=vmem((nh, PAIR, model), BF),
        wf_in=vmem((3, width, model), BF), wr_in=vmem((1, model), BF),
        gu=vmem((2, width, hidden), F32), dt=vmem((width, hidden), F32),
        wf=vmem((3 * wide, model), BF), fq=vmem((tokens, wide), BF),
        fkt=vmem((wide, tokens), BF), ogt=vmem((wide, tokens), BF),
        col=vmem((tokens, width), BF), two=vmem((parts, tokens, 2 * LANES), BF),
        hk=vmem((parts, tokens, LANES), BF),
        guw=vmem((parts, wide, 2 * LANES), BF), dth=vmem((wide, hidden), BF),
        g=vmem((max(3 * width, chunk * n), LANES), F32),
        total=vmem((max(3 * width, chunk * n), hidden), F32),
        ag=vmem((wide, 2 * hidden), BF), ad=vmem((width, hidden), BF),
        part=vmem((parts, 2, outer, chunk, LANES), BF), xin=vmem((parts, outer, chunk, LANES), BF),
        half=vmem((parts, outer, chunk, LANES), BF), zin=vmem((parts, outer - 1, chunk, LANES), BF),
        res=vmem((parts, 2, outer, chunk, LANES), BF),
        eg_in=vmem((model // LANES, LANES), F32), fg_in=vmem((model // LANES, LANES), F32),
        eg=vmem((1, model), F32), fg=vmem((1, model), F32), done=vmem((tokens, width), BF),
        local=dma((STEPS + 9,)), put=dma((tokens // BLK,)),
        xs=dma((STEPS, n - 1)), xr=dma((STEPS, n - 1)), ms=dma((n - 1,)), mr=dma((n - 1,)),
        ws=dma((3, 4)), wr=dma((3, 4)), ss=dma((STEPS, nh - 1)), sr=dma((STEPS, nh - 1)),
        gs=dma((3, PAIR // CHUNK)), gr=dma((3, PAIR // CHUNK)),
        ps=dma((parts,)), pr=dma((parts,)), zs=dma((parts, outer - 1)), zr=dma((parts, outer - 1)),
        rs=dma((parts, outer)), rr=dma((parts, outer)),
        fs=dma((parts, outer - 1)), fr=dma((parts, outer - 1)),
    )
    return sizes


def gradient_sum(n, width, s, side, lane, compute, during):
    seq = lax.axis_index("seq")
    outer_count = n // 2
    inner, outer = lax.rem(seq, 2), lax.div(seq, 2)
    parts = s.part.shape[0]
    chunk = s.part.shape[3]
    steps = range(1, outer_count)

    def plan(part):
        mine = s.res.at[part, inner, outer]
        theirs = [s.res.at[part, inner, lax.rem(outer + outer_count - t, outer_count)] for t in steps]
        return types.SimpleNamespace(
            x=remote(s.part.at[part, 1 - inner], s.xin.at[part], s.ps.at[part], s.pr.at[part], side),
            z=[
                remote(
                    s.half.at[part, lax.rem(outer + t, outer_count)], s.zin.at[part, t - 1],
                    s.zs.at[part, t - 1], s.zr.at[part, t - 1], lane[t - 1],
                )
                for t in steps
            ],
            r=[
                remote(mine, mine, s.rs.at[part, t], s.rr.at[part, t], to)
                for t, to in enumerate(lane + [side])
            ],
            f=[
                remote(theirs[t - 1], theirs[t - 1], s.fs.at[part, t - 1], s.fr.at[part, t - 1], side)
                for t in steps
            ],
        )

    plans = [plan(part) for part in range(parts)]

    def stage_x(part):
        plans[part].x.start()

    def stage_z(part):
        plans[part].x.wait_recv()
        for o in range(outer_count):
            s.half[part, o] = (
                s.part[part, inner, o].astype(F32) + s.xin[part, o].astype(F32)
            ).astype(BF)
        for copy in plans[part].z:
            copy.start()

    def stage_r(part):
        total = s.half[part, outer].astype(F32)
        for t, copy in enumerate(plans[part].z):
            copy.wait_recv()
            total = total + s.zin[part, t].astype(F32)
        s.res[part, inner, outer] = total.astype(BF)
        for copy in plans[part].r:
            copy.start()

    def stage_f(part):
        for t in steps:
            plans[part].r[t - 1].wait_recv()
            plans[part].f[t - 1].start()

    stages = [stage_x, stage_z, stage_r, stage_f]
    for tick in range(parts + len(stages) - 1):
        if tick < parts:
            compute(tick)
        for which, stage in enumerate(stages):
            if 0 <= tick - which < parts:
                stage(tick - which)
        if tick == parts - 1:
            during()
    for part in range(parts):
        plans[part].r[-1].wait_recv()
        for copy in plans[part].f:
            copy.wait_recv()
        cut = slice(part * LANES, (part + 1) * LANES)
        for i in range(2):
            for o in range(outer_count):
                at = (i * outer_count + o) * chunk
                s.total[at : at + chunk, cut] = s.res[part, i, o].astype(F32)
    for part in range(parts):
        plans[part].x.wait_send()
        for copy in plans[part].z + plans[part].r + plans[part].f:
            copy.wait_send()


def whole_kernel(
    n, nh, names, dest_ref, image_ref, x_ref, wqkv_ref, wo_ref, eg_ref, fg_ref, wf_ref, wr_ref,
    gu_ref, dt_ref, o_ref, *scratch,
):
    s = types.SimpleNamespace(**dict(zip(names, scratch)))
    seq, head = lax.axis_index("seq"), lax.axis_index("head")
    partner = head + 1 - 2 * lax.rem(head, 2)
    peer = lax.rem(head + nh // 2, nh)
    targets = others(n, seq)
    mates = others(nh, head)
    outer_count = n // 2
    inner, outer = lax.rem(seq, 2), lax.div(seq, 2)
    side = (outer * 2 + 1 - inner, head)
    lane = [(lax.rem(outer + t, outer_count) * 2 + inner, head) for t in range(1, outer_count)]
    model = x_ref.shape[-1]
    width, hidden = gu_ref.shape[1:]
    wide = s.fq.shape[1]
    parts = hidden // LANES
    tokens = nh * PAIR
    held = [getattr(s, f"held{c}") for c in range(STEPS)]
    out = [getattr(s, f"out{c}") for c in range(STEPS)]
    arrived = [getattr(s, f"in{c}") for c in range(STEPS)]
    chosen = [getattr(s, f"chosen{c}") for c in range(STEPS)]
    rows = held[0].shape[1]
    per_block = nh // 2

    barrier = pltpu.get_barrier_semaphore()
    greeted = [(to, head) for to in targets] + [(seq, to) for to in mates]
    for device in greeted:
        pl.semaphore_signal(barrier, inc=1, device_id=device, device_id_type=MESH)

    fetch = [
        pltpu.make_async_copy(x_ref.at[:, lax.rem(head, per_block), c], held[c], s.local.at[c])
        for c in range(STEPS)
    ]
    weights_in = [
        pltpu.make_async_copy(wqkv_ref, s.w.at[0:3, head], s.local.at[STEPS]),
        pltpu.make_async_copy(wo_ref, s.w.at[3, head], s.local.at[STEPS + 1]),
    ]
    late = [
        pltpu.make_async_copy(src, dst, s.local.at[STEPS + 2 + which])
        for which, (src, dst) in enumerate(
            [(wf_ref, s.wf_in), (wr_ref, s.wr_in), (gu_ref, s.gu), (dt_ref, s.dt)]
        )
    ]
    gains_in = [
        pltpu.make_async_copy(src, dst, s.local.at[STEPS + 7 + which])
        for which, (src, dst) in enumerate([(eg_ref, s.eg_in), (fg_ref, s.fg_in)])
    ]
    for copy in fetch[:1] + weights_in + fetch[1:] + late + gains_in:
        copy.start()

    my_block = lax.div(head, per_block)
    pairs = dest_ref.shape[0] // 2
    firsts = [dest_ref[2 * i] for i in range(pairs)]
    sames = [(image_ref[2 * i] == image_ref[2 * i + 1]).astype(jnp.int32) for i in range(pairs)]
    homes = [lax.div(jnp.maximum(d, 0), BLK_DEV) for d in firsts]
    slots = []
    for i, d in enumerate(firsts):
        slots.append(2 * i + lax.rem(jnp.maximum(d, 0) + my_block, 2))
    marks = [
        2 * lax.div(lax.rem(jnp.maximum(d, 0), BLK_DEV), 2) + same for d, same in zip(firsts, sames)
    ]

    def lookup(target):
        slot, code = jnp.int32(0), jnp.int32(-1)
        for i, d in enumerate(firsts):
            hit = jnp.logical_and(d >= 0, homes[i] == target)
            slot = jnp.where(hit, slots[i], slot)
            code = jnp.where(hit, marks[i], code)
        return slot, code

    found = [lookup(to) for to in targets + [seq]]
    for step, to in enumerate(targets):
        s.meta[step] = jnp.full((1, LANES), found[step][1], jnp.int32)
    s.meta_in[seq] = jnp.full((1, LANES), found[-1][1], jnp.int32)

    def pick(c):
        fetch[c].wait()
        for step in range(n - 1):
            out[c][step] = held[c][found[step][0]]
        arrived[c][seq] = held[c][found[-1][0]]

    meta_copies = [
        remote(s.meta.at[step], s.meta_in.at[seq], s.ms.at[step], s.mr.at[step], (to, head))
        for step, to in enumerate(targets)
    ]
    x_copies = [
        [
            remote(out[c].at[step], arrived[c].at[seq], s.xs.at[c, step], s.xr.at[c, step], (to, head))
            for step, to in enumerate(targets)
        ]
        for c in range(STEPS)
    ]
    to_peer = [
        remote(s.w.at[m, head], s.w.at[m, head], s.ws.at[0, m], s.wr.at[0, m], (seq, peer))
        for m in range(4)
    ]
    to_partner = [
        remote(s.w.at[m, head], s.w.at[m, head], s.ws.at[1, m], s.wr.at[1, m], (seq, partner))
        for m in range(4)
    ]
    passed = [
        remote(s.w.at[m, peer], s.w.at[m, peer], s.ws.at[2, m], s.wr.at[2, m], (seq, partner))
        for m in range(4)
    ]
    pick(0)
    pl.semaphore_wait(barrier, len(greeted))
    for copy in meta_copies + x_copies[0]:
        copy.start()
    for copy in weights_in:
        copy.wait()
    for copy in to_peer + to_partner:
        copy.start()
    for c in range(1, STEPS):
        pick(c)
        for copy in x_copies[c]:
            copy.start()

    s.wf[...] = jnp.zeros_like(s.wf)
    s.v[...] = jnp.ones_like(s.v)
    s.guw[...] = jnp.zeros_like(s.guw)
    s.dth[...] = jnp.zeros_like(s.dth)
    s.g[...] = jnp.zeros_like(s.g)
    s.ag[...] = jnp.zeros_like(s.ag)
    for copy in late + gains_in:
        copy.wait()
    for src, dst in ((s.eg_in, s.eg), (s.fg_in, s.fg)):
        for which in range(model // LANES):
            dst[:, which * LANES : (which + 1) * LANES] = src[which : which + 1]
    for which in range(3):
        s.wf[which * wide : which * wide + width] = s.wf_in[which]
    rate_at = 2 * wide + width
    s.wf[rate_at : rate_at + 16] = jnp.broadcast_to(s.wr_in[...], (16, model))
    s.dth[:width] = s.dt[...].astype(BF)
    for part in range(parts):
        cut = slice(part * LANES, (part + 1) * LANES)
        s.guw[part, :width, :LANES] = s.gu[0, :, cut].astype(BF)
        s.guw[part, :width, LANES:] = s.gu[1, :, cut].astype(BF)

    for copy in meta_copies:
        copy.wait_recv()
    spread = pltpu.make_async_copy(s.meta_in, s.codes, s.local.at[STEPS + 6])
    spread.start()
    spread.wait()
    sources = [jnp.int32(0)] * nh
    same = jnp.int32(0)
    for source in range(n):
        code = s.codes[source, 0, 0]
        place = lax.div(jnp.maximum(code, 0), 2)
        for p in range(nh):
            sources[p] = jnp.where(jnp.logical_and(code >= 0, place == p), source, sources[p])
        mine = jnp.logical_and(code >= 0, place == head)
        same = jnp.where(mine, lax.rem(jnp.maximum(code, 0), 2), same)

    swaps = [
        [
            remote(
                chosen[c].at[to], s.pair.at[lax.div(head, per_block), c, lax.rem(head, per_block)],
                s.ss.at[c, step], s.sr.at[c, step], (seq, to),
            )
            for step, to in enumerate(mates)
        ]
        for c in range(STEPS)
    ]

    def swap(c):
        for copy in x_copies[c]:
            copy.wait_recv()
        for p in range(nh):
            chosen[c][p] = arrived[c][sources[p]]
        for copy in swaps[c]:
            copy.start()
        s.pair[lax.div(head, per_block), c, lax.rem(head, per_block)] = chosen[c][head]

    def matrix(m):
        return s.w[m].reshape(nh * width, model)

    run = per_block * rows

    def project(c):
        for copy in swaps[c]:
            copy.wait_recv()
        taken = jnp.concatenate([s.pair[b, c].reshape(run, model) for b in range(2)], axis=0)
        normed = norm_rows(taken, s.eg[...])
        values = [dot_nt(normed, matrix(m)).astype(BF) for m in range(3)]
        values[0] = values[0] * BF(HDIM ** (-0.5))
        for b in range(2):
            at = b * BLK + c * run
            s.q[at : at + run] = values[0][b * run : (b + 1) * run]
            s.k[at : at + run] = values[1][b * run : (b + 1) * run]
            for slab in range(model // LANES):
                s.v[at : at + run, 2 * slab * LANES : (2 * slab + 1) * LANES] = values[2][
                    b * run : (b + 1) * run, slab * LANES : (slab + 1) * LANES
                ]

    def forward(m):
        to_peer[m].wait_recv()
        passed[m].start()

    for c in range(STEPS):
        swap(c)
        if c == STEPS - 2:
            for m in range(4):
                forward(m)
            for m in range(3):
                to_partner[m].wait_recv()
                passed[m].wait_recv()
            for early in range(c):
                project(early)
    project(STEPS - 2)
    project(STEPS - 1)
    to_partner[3].wait_recv()
    passed[3].wait_recv()

    apart = jnp.where(same > 0, 0.0, -1e30).astype(F32)
    key_block = lax.broadcasted_iota(jnp.int32, (1, PAIR), 1) // BLK
    first = lax.broadcasted_iota(jnp.int32, (CHUNK, LANES), 1) < HDIM
    chunks = PAIR // CHUNK

    def emb_copies(i):
        at = pl.ds(pl.multiple_of(i * CHUNK, CHUNK), CHUNK)
        mine, theirs = s.emb.at[head, at], s.emb.at[peer, at]
        return types.SimpleNamespace(
            peer=remote(mine, mine, s.gs.at[0, i], s.gr.at[0, i], (seq, peer)),
            partner=remote(mine, mine, s.gs.at[1, i], s.gr.at[1, i], (seq, partner)),
            across=remote(theirs, theirs, s.gs.at[2, i], s.gr.at[2, i], (seq, partner)),
        )

    per_chunk = CHUNK // run

    def attend(i):
        at = pl.ds(pl.multiple_of(i * CHUNK, CHUNK), CHUNK)
        block = lax.div(i, BLK // CHUNK)
        bias = jnp.where(key_block == block, 0.0, apart)
        for slab in range(model // LANES):
            columns = slice(slab * LANES, (slab + 1) * LANES)
            query = s.q[at, columns]
            nothing = jnp.zeros_like(query)
            both = jnp.concatenate(
                [jnp.where(first, query, nothing), jnp.where(first, nothing, query)], axis=0
            )
            scores = dot_nt(both, s.k[:, columns]) + bias
            top = jnp.max(scores, axis=-1, keepdims=True)
            weights = jnp.exp(scores - top).astype(BF)
            mixed = dot(weights, s.v[:, 2 * slab * LANES : 2 * (slab + 1) * LANES])
            mixed = mixed[:, :LANES] * (1.0 / mixed[:, LANES:])
            s.a[:, columns] = jnp.where(first, mixed[:CHUNK], mixed[CHUNK:]).astype(BF)
        mixed = dot(s.a[...], matrix(3))
        low = lax.rem(i, BLK // CHUNK) * per_chunk
        taken = s.pair[block, pl.ds(low, per_chunk)].reshape(CHUNK, model)
        s.emb[head, at] = (taken.astype(F32) + mixed).astype(BF)

    scale = RATE_SCALE * (tokens * n) ** (-0.5)

    def fast_project(owner, i):
        at = pl.ds(pl.multiple_of(owner * PAIR + i * CHUNK, CHUNK), CHUNK)
        normed = norm_rows(s.emb[owner, pl.ds(i * CHUNK, CHUNK)], s.fg[...])
        mapped = dot_nt(normed, s.wf[...])
        s.fq[at] = mapped[:, :wide].astype(BF)
        key = mapped[:, wide : 2 * wide].astype(BF)
        s.fkt[:, at] = key.T
        value = mapped[:, 2 * wide :].astype(BF).astype(F32)
        before = mapped[:, rate_at : rate_at + 1]
        soft = jnp.maximum(before, 0.0) + jnp.log1p(jnp.exp(-jnp.abs(before)))
        back = (-(scale * soft) * value).astype(BF)
        s.ogt[:, at] = back.T
        for part in range(parts):
            both = dot(key, s.guw[part])
            gate, up = both[:, :LANES], both[:, LANES:]
            grad = dot(back, s.dth[:, part * LANES : (part + 1) * LANES])
            sig = jax.nn.sigmoid(gate)
            silu = gate * sig
            s.hk[part, at] = (silu * up).astype(BF)
            s.two[part, at, :LANES] = (grad * up * sig * (1.0 + gate * (1.0 - sig))).astype(BF)
            s.two[part, at, LANES:] = (grad * silu).astype(BF)

    across = lax.rem(partner + nh // 2, nh)

    def take_partner(i):
        emb_copies(i).partner.wait_recv()

    def take_peer(i):
        copies = emb_copies(i)
        copies.peer.wait_recv()
        copies.across.start()

    def own_chunk(i, carry):
        attend(i)
        copies = emb_copies(i)
        copies.peer.start()
        copies.partner.start()

        def one(which, inside):
            at = i - which

            @pl.when(at >= 0)
            def _():
                @pl.when(which == 1)
                def _():
                    take_partner(at)

                @pl.when(which == 2)
                def _():
                    take_peer(at)

                owner = jnp.where(which == 0, head, jnp.where(which == 1, partner, peer))
                fast_project(owner, at)

            return inside

        return lax.fori_loop(0, 3, one, carry)

    lax.fori_loop(0, chunks, own_chunk, 0)
    take_partner(chunks - 1)
    fast_project(partner, chunks - 1)
    emb_copies(0).across.wait_recv()
    fast_project(across, 0)
    take_peer(chunks - 2)
    fast_project(peer, chunks - 2)
    for i in range(1, chunks - 1):
        emb_copies(i).across.wait_recv()
        fast_project(across, i)
    take_peer(chunks - 1)
    fast_project(peer, chunks - 1)
    emb_copies(chunks - 1).across.wait_recv()
    fast_project(across, chunks - 1)

    def compute(part):
        one = dot(s.fkt[...], s.two[part])
        other = dot(s.ogt[...], s.hk[part])
        s.g[0:width] = one[:width, :LANES]
        s.g[width : 2 * width] = one[:width, LANES:]
        s.g[2 * width : 3 * width] = other[:width]
        chunk = s.part.shape[3]
        for i in range(2):
            for o in range(outer_count):
                at = (i * outer_count + o) * chunk
                s.part[part, i, o] = s.g[at : at + chunk].astype(BF)

    def during():
        for which in range(model // width):

            @pl.when(head == which)
            def _():
                for owner in range(nh):
                    at = owner * PAIR
                    s.col[at : at + PAIR] = s.emb[owner, :, which * width : (which + 1) * width]

    gradient_sum(n, width, s, side, lane, compute, during)

    for which in range(2):
        start = s.gu[which]
        fresh = renorm(start - s.total[which * width : (which + 1) * width], start, 1)
        s.ag[:width, which * hidden : (which + 1) * hidden] = fresh.astype(BF)
    start = s.dt[...]
    s.ad[...] = renorm(start - s.total[2 * width : 3 * width], start, 0).astype(BF)

    def put(unit):
        at = pl.ds(unit * BLK, BLK)
        return pltpu.make_async_copy(s.done.at[at], o_ref.at[at], s.put.at[unit])

    def final(unit, carry):
        base = pl.multiple_of(unit * BLK, BLK)
        at = pl.ds(base, BLK)
        both = dot(s.fq[at], s.ag[...])
        gate = both[:, :hidden]
        inside = (gate * jax.nn.sigmoid(gate) * both[:, hidden:]).astype(BF)
        done = (s.col[at].astype(F32) + dot_nt(inside, s.ad[...])).astype(BF)
        for c in range(STEPS):
            for which in range(per_block):
                low = (c * per_block + which) * rows
                to = pl.multiple_of(base + which * STEPS * rows + c * rows, rows)
                s.done[pl.ds(to, rows)] = done[low : low + rows]
        put(unit).start()
        return carry

    lax.fori_loop(0, tokens // BLK, final, 0, unroll=2)
    for unit in range(tokens // BLK):
        put(unit).wait()

    for copy in meta_copies + to_peer + to_partner + passed:
        copy.wait_send()
    for group in x_copies + swaps:
        for copy in group:
            copy.wait_send()
    for i in range(chunks):
        copies = emb_copies(i)
        for copy in (copies.peer, copies.partner, copies.across):
            copy.wait_send()


def on_device(
    patches,
    slot_image,
    slot_dest,
    enc_gain,
    w_qkv,
    w_out,
    fast_gain,
    w_fast,
    w_rate,
    fast_gate_up,
    fast_down,
):
    n = lax.axis_size("seq")
    nh = lax.axis_size("head")
    model = patches.shape[1]
    slots = slot_dest.shape[0]
    width, hidden = fast_gate_up.shape[2:]
    part = PAIR // nh
    sizes = layout(n, nh, slots, model, width, hidden)
    return pl.pallas_call(
        functools.partial(whole_kernel, n, nh, tuple(sizes)),
        out_shape=jax.ShapeDtypeStruct((nh * PAIR, width), patches.dtype),
        in_specs=[SMEM, SMEM] + [ANY] * 9,
        out_specs=ANY,
        scratch_shapes=list(sizes.values()),
        compiler_params=pltpu.CompilerParams(
            collective_id=1, has_side_effects=True, vmem_limit_bytes=60 * 1024 * 1024
        ),
        name="encode_and_update",
    )(
        slot_dest,
        slot_image,
        patches.reshape(slots, BLK // part, STEPS, part // STEPS, model),
        jnp.swapaxes(w_qkv, 1, 2),
        w_out,
        enc_gain.reshape(model // LANES, LANES),
        fast_gain.reshape(model // LANES, LANES),
        jnp.swapaxes(w_fast, 1, 2),
        w_rate.T,
        fast_gate_up[0],
        fast_down[0].T,
    )


def solution(mesh):
    in_specs = (
        P("seq", None),
        P("seq"),
        P("seq"),
        P(),
        P(None, None, "head"),
        P("head", None),
        P(),
        P(None, None, "head"),
        P(None, "head"),
        P("head", None, None, None),
        P("head", None, None),
    )
    out_specs = P("seq", "head")
    return jax.shard_map(
        on_device, mesh=mesh, in_specs=in_specs, out_specs=out_specs, check_vma=False
    )
```

```python
import functools
import types

import jax
import jax.numpy as jnp
from jax import lax
from jax.experimental import pallas as pl
from jax.experimental.pallas import tpu as pltpu
from jax.sharding import PartitionSpec as P

HDIM = 64
BLK = 256
BLK_DEV = 8
PAIR = 2 * BLK
EPSILON = 1e-06
RATE_SCALE = 0.1
LANES = 128
STEPS = 4
CHUNK = 128
UNIT = 256
MESH = pl.DeviceIdType.MESH
VMEM = pl.BlockSpec(memory_space=pltpu.VMEM)
SMEM = pl.BlockSpec(memory_space=pltpu.SMEM)
ANY = pl.BlockSpec(memory_space=pl.ANY)
NT = (((1,), (1,)), ((), ()))
BF = jnp.bfloat16
F32 = jnp.float32


def remote(src, dst, send, recv, device):
    return pltpu.make_async_remote_copy(
        src_ref=src, dst_ref=dst, send_sem=send, recv_sem=recv, device_id=device, device_id_type=MESH
    )


def others(axis_size, me):
    return [lax.rem(me + step, axis_size) for step in range(1, axis_size)]


def dot(a, b):
    return jnp.dot(a, b, preferred_element_type=F32)


def dot_nt(a, b):
    return lax.dot_general(a, b, NT, preferred_element_type=F32)


def norm_rows(values, gain):
    wide = values.astype(F32)
    factor = lax.rsqrt(jnp.mean(wide * wide, axis=-1, keepdims=True) + EPSILON)
    return (wide * factor * gain).astype(BF)


def renorm(updated, initial, axis):
    target_norm = jnp.sqrt(jnp.sum(initial * initial, axis=axis, keepdims=True))
    return (
        updated
        * target_norm
        * lax.rsqrt(jnp.sum(updated * updated, axis=axis, keepdims=True) + EPSILON)
    )


def layout(n, nh, slots, model, width, hidden):
    vmem, dma = pltpu.VMEM, pltpu.SemaphoreType.DMA
    part = PAIR // nh
    rows = part // STEPS
    wide = LANES * (-(-width // LANES))
    tokens = nh * PAIR
    parts = hidden // LANES
    chunk = 8 * (-(-3 * width // (8 * n)))
    outer = n // 2
    sizes = {}
    for c in range(STEPS):
        sizes[f"held{c}"] = vmem((slots, rows, model), BF)
        sizes[f"out{c}"] = vmem((n, rows, model), BF)
        sizes[f"in{c}"] = vmem((n, rows, model), BF)
        sizes[f"chosen{c}"] = vmem((nh, rows, model), BF)
    sizes.update(
        meta=vmem((n, 1, LANES), jnp.int32), meta_in=vmem((n, 1, LANES), jnp.int32),
        codes=pltpu.SMEM((n, 1, LANES), jnp.int32),
        w=vmem((4, nh, width, model), BF),
        pair=vmem((2, STEPS, nh // 2, rows, model), BF),
        q=vmem((PAIR, model), BF), k=vmem((PAIR, model), BF), v=vmem((PAIR, 2 * model), BF),
        a=vmem((CHUNK, model), BF), emb=vmem((nh, PAIR, model), BF),
        wf_in=vmem((3, width, model), BF), wr_in=vmem((1, model), BF),
        gu=vmem((2, width, hidden), F32), dt=vmem((width, hidden), F32),
        wf=vmem((3 * wide, model), BF), fq=vmem((tokens, wide), BF),
        fkt=vmem((wide, tokens), BF), ogt=vmem((wide, tokens), BF),
        col=vmem((tokens, width), BF), two=vmem((parts, tokens, 2 * LANES), BF),
        hk=vmem((parts, tokens, LANES), BF),
        guw=vmem((parts, wide, 2 * LANES), BF), dth=vmem((wide, hidden), BF),
        g=vmem((max(3 * width, chunk * n), LANES), F32),
        total=vmem((max(3 * width, chunk * n), hidden), F32),
        ag=vmem((wide, 2 * hidden), BF), ad=vmem((width, hidden), BF),
        part=vmem((parts, 2, outer, chunk, LANES), BF), xin=vmem((parts, outer, chunk, LANES), BF),
        half=vmem((parts, outer, chunk, LANES), BF), zin=vmem((parts, outer - 1, chunk, LANES), BF),
        res=vmem((parts, 2, outer, chunk, LANES), BF),
        eg_in=vmem((model // LANES, LANES), F32), fg_in=vmem((model // LANES, LANES), F32),
        eg=vmem((1, model), F32), fg=vmem((1, model), F32), done=vmem((tokens, width), BF),
        local=dma((STEPS + 9,)), put=dma((tokens // BLK,)),
        xs=dma((STEPS, n - 1)), xr=dma((STEPS, n - 1)), ms=dma((n - 1,)), mr=dma((n - 1,)),
        ws=dma((3, 4)), wr=dma((3, 4)), ss=dma((STEPS, nh - 1)), sr=dma((STEPS, nh - 1)),
        gs=dma((3, PAIR // CHUNK)), gr=dma((3, PAIR // CHUNK)),
        ps=dma((parts,)), pr=dma((parts,)), zs=dma((parts, outer - 1)), zr=dma((parts, outer - 1)),
        rs=dma((parts, outer)), rr=dma((parts, outer)),
        fs=dma((parts, outer - 1)), fr=dma((parts, outer - 1)),
    )
    return sizes


def gradient_sum(n, width, s, side, lane, compute, during):
    seq = lax.axis_index("seq")
    outer_count = n // 2
    inner, outer = lax.rem(seq, 2), lax.div(seq, 2)
    parts = s.part.shape[0]
    chunk = s.part.shape[3]
    steps = range(1, outer_count)

    def plan(part):
        mine = s.res.at[part, inner, outer]
        theirs = [s.res.at[part, inner, lax.rem(outer + outer_count - t, outer_count)] for t in steps]
        return types.SimpleNamespace(
            x=remote(s.part.at[part, 1 - inner], s.xin.at[part], s.ps.at[part], s.pr.at[part], side),
            z=[
                remote(
                    s.half.at[part, lax.rem(outer + t, outer_count)], s.zin.at[part, t - 1],
                    s.zs.at[part, t - 1], s.zr.at[part, t - 1], lane[t - 1],
                )
                for t in steps
            ],
            r=[
                remote(mine, mine, s.rs.at[part, t], s.rr.at[part, t], to)
                for t, to in enumerate(lane + [side])
            ],
            f=[
                remote(theirs[t - 1], theirs[t - 1], s.fs.at[part, t - 1], s.fr.at[part, t - 1], side)
                for t in steps
            ],
        )

    plans = [plan(part) for part in range(parts)]

    def stage_x(part):
        plans[part].x.start()

    def stage_z(part):
        plans[part].x.wait_recv()
        for o in range(outer_count):
            s.half[part, o] = (
                s.part[part, inner, o].astype(F32) + s.xin[part, o].astype(F32)
            ).astype(BF)
        for copy in plans[part].z:
            copy.start()

    def stage_r(part):
        total = s.half[part, outer].astype(F32)
        for t, copy in enumerate(plans[part].z):
            copy.wait_recv()
            total = total + s.zin[part, t].astype(F32)
        s.res[part, inner, outer] = total.astype(BF)
        for copy in plans[part].r:
            copy.start()

    def stage_f(part):
        for t in steps:
            plans[part].r[t - 1].wait_recv()
            plans[part].f[t - 1].start()

    for part in range(parts):
        compute(part)
        stage_x(part)
    for part in range(parts):
        stage_z(part)
    during()
    for part in range(parts):
        stage_r(part)
    for part in range(parts):
        stage_f(part)
    for part in range(parts):
        plans[part].r[-1].wait_recv()
        for copy in plans[part].f:
            copy.wait_recv()
        cut = slice(part * LANES, (part + 1) * LANES)
        for i in range(2):
            for o in range(outer_count):
                at = (i * outer_count + o) * chunk
                s.total[at : at + chunk, cut] = s.res[part, i, o].astype(F32)
    for part in range(parts):
        plans[part].x.wait_send()
        for copy in plans[part].z + plans[part].r + plans[part].f:
            copy.wait_send()


def whole_kernel(
    n, nh, names, dest_ref, image_ref, x_ref, wqkv_ref, wo_ref, eg_ref, fg_ref, wf_ref, wr_ref,
    gu_ref, dt_ref, o_ref, *scratch,
):
    s = types.SimpleNamespace(**dict(zip(names, scratch)))
    seq, head = lax.axis_index("seq"), lax.axis_index("head")
    partner = head + 1 - 2 * lax.rem(head, 2)
    peer = lax.rem(head + nh // 2, nh)
    targets = others(n, seq)
    mates = others(nh, head)
    outer_count = n // 2
    inner, outer = lax.rem(seq, 2), lax.div(seq, 2)
    side = (outer * 2 + 1 - inner, head)
    lane = [(lax.rem(outer + t, outer_count) * 2 + inner, head) for t in range(1, outer_count)]
    model = x_ref.shape[-1]
    width, hidden = gu_ref.shape[1:]
    wide = s.fq.shape[1]
    parts = hidden // LANES
    tokens = nh * PAIR
    held = [getattr(s, f"held{c}") for c in range(STEPS)]
    out = [getattr(s, f"out{c}") for c in range(STEPS)]
    arrived = [getattr(s, f"in{c}") for c in range(STEPS)]
    chosen = [getattr(s, f"chosen{c}") for c in range(STEPS)]
    rows = held[0].shape[1]
    per_block = nh // 2

    barrier = pltpu.get_barrier_semaphore()
    greeted = [(to, head) for to in targets] + [(seq, to) for to in mates]
    for device in greeted:
        pl.semaphore_signal(barrier, inc=1, device_id=device, device_id_type=MESH)

    fetch = [
        pltpu.make_async_copy(x_ref.at[:, lax.rem(head, per_block), c], held[c], s.local.at[c])
        for c in range(STEPS)
    ]
    weights_in = [
        pltpu.make_async_copy(wqkv_ref, s.w.at[0:3, head], s.local.at[STEPS]),
        pltpu.make_async_copy(wo_ref, s.w.at[3, head], s.local.at[STEPS + 1]),
    ]
    late = [
        pltpu.make_async_copy(src, dst, s.local.at[STEPS + 2 + which])
        for which, (src, dst) in enumerate(
            [(wf_ref, s.wf_in), (wr_ref, s.wr_in), (gu_ref, s.gu), (dt_ref, s.dt)]
        )
    ]
    gains_in = [
        pltpu.make_async_copy(src, dst, s.local.at[STEPS + 7 + which])
        for which, (src, dst) in enumerate([(eg_ref, s.eg_in), (fg_ref, s.fg_in)])
    ]
    for copy in fetch[:1] + weights_in + fetch[1:] + late + gains_in:
        copy.start()

    my_block = lax.div(head, per_block)
    pairs = dest_ref.shape[0] // 2
    firsts = [dest_ref[2 * i] for i in range(pairs)]
    sames = [(image_ref[2 * i] == image_ref[2 * i + 1]).astype(jnp.int32) for i in range(pairs)]
    homes = [lax.div(jnp.maximum(d, 0), BLK_DEV) for d in firsts]
    slots = []
    for i, d in enumerate(firsts):
        slots.append(2 * i + lax.rem(jnp.maximum(d, 0) + my_block, 2))
    marks = [
        2 * lax.div(lax.rem(jnp.maximum(d, 0), BLK_DEV), 2) + same for d, same in zip(firsts, sames)
    ]

    def lookup(target):
        slot, code = jnp.int32(0), jnp.int32(-1)
        for i, d in enumerate(firsts):
            hit = jnp.logical_and(d >= 0, homes[i] == target)
            slot = jnp.where(hit, slots[i], slot)
            code = jnp.where(hit, marks[i], code)
        return slot, code

    found = [lookup(to) for to in targets + [seq]]
    for step, to in enumerate(targets):
        s.meta[step] = jnp.full((1, LANES), found[step][1], jnp.int32)
    s.meta_in[seq] = jnp.full((1, LANES), found[-1][1], jnp.int32)

    def pick(c):
        fetch[c].wait()
        for step in range(n - 1):
            out[c][step] = held[c][found[step][0]]
        arrived[c][seq] = held[c][found[-1][0]]

    meta_copies = [
        remote(s.meta.at[step], s.meta_in.at[seq], s.ms.at[step], s.mr.at[step], (to, head))
        for step, to in enumerate(targets)
    ]
    x_copies = [
        [
            remote(out[c].at[step], arrived[c].at[seq], s.xs.at[c, step], s.xr.at[c, step], (to, head))
            for step, to in enumerate(targets)
        ]
        for c in range(STEPS)
    ]
    to_peer = [
        remote(s.w.at[m, head], s.w.at[m, head], s.ws.at[0, m], s.wr.at[0, m], (seq, peer))
        for m in range(4)
    ]
    to_partner = [
        remote(s.w.at[m, head], s.w.at[m, head], s.ws.at[1, m], s.wr.at[1, m], (seq, partner))
        for m in range(4)
    ]
    passed = [
        remote(s.w.at[m, peer], s.w.at[m, peer], s.ws.at[2, m], s.wr.at[2, m], (seq, partner))
        for m in range(4)
    ]
    pick(0)
    pl.semaphore_wait(barrier, len(greeted))
    far_first = sorted(range(n - 1), key=lambda step: abs(step + 1 - n // 2))
    for copy in meta_copies + [x_copies[0][step] for step in far_first]:
        copy.start()
    for copy in weights_in:
        copy.wait()
    for copy in to_peer + to_partner:
        copy.start()
    for c in range(1, STEPS):
        pick(c)
        for step in far_first:
            x_copies[c][step].start()

    s.wf[...] = jnp.zeros_like(s.wf)
    s.v[...] = jnp.ones_like(s.v)
    s.guw[...] = jnp.zeros_like(s.guw)
    s.dth[...] = jnp.zeros_like(s.dth)
    s.g[...] = jnp.zeros_like(s.g)
    s.ag[...] = jnp.zeros_like(s.ag)
    for copy in late + gains_in:
        copy.wait()
    for src, dst in ((s.eg_in, s.eg), (s.fg_in, s.fg)):
        for which in range(model // LANES):
            dst[:, which * LANES : (which + 1) * LANES] = src[which : which + 1]
    for which in range(3):
        s.wf[which * wide : which * wide + width] = s.wf_in[which]
    rate_at = 2 * wide + width
    s.wf[rate_at : rate_at + 16] = jnp.broadcast_to(s.wr_in[...], (16, model))
    s.dth[:width] = s.dt[...].astype(BF)
    for part in range(parts):
        cut = slice(part * LANES, (part + 1) * LANES)
        s.guw[part, :width, :LANES] = s.gu[0, :, cut].astype(BF)
        s.guw[part, :width, LANES:] = s.gu[1, :, cut].astype(BF)

    for copy in meta_copies:
        copy.wait_recv()
    spread = pltpu.make_async_copy(s.meta_in, s.codes, s.local.at[STEPS + 6])
    spread.start()
    spread.wait()
    sources = [jnp.int32(0)] * nh
    same = jnp.int32(0)
    for source in range(n):
        code = s.codes[source, 0, 0]
        place = lax.div(jnp.maximum(code, 0), 2)
        for p in range(nh):
            sources[p] = jnp.where(jnp.logical_and(code >= 0, place == p), source, sources[p])
        mine = jnp.logical_and(code >= 0, place == head)
        same = jnp.where(mine, lax.rem(jnp.maximum(code, 0), 2), same)

    swaps = [
        [
            remote(
                chosen[c].at[to], s.pair.at[lax.div(head, per_block), c, lax.rem(head, per_block)],
                s.ss.at[c, step], s.sr.at[c, step], (seq, to),
            )
            for step, to in enumerate(mates)
        ]
        for c in range(STEPS)
    ]

    def swap(c):
        for copy in x_copies[c]:
            copy.wait_recv()
        for p in range(nh):
            chosen[c][p] = arrived[c][sources[p]]
        for copy in swaps[c]:
            copy.start()
        s.pair[lax.div(head, per_block), c, lax.rem(head, per_block)] = chosen[c][head]

    def matrix(m):
        return s.w[m].reshape(nh * width, model)

    run = per_block * rows

    def project(c):
        for copy in swaps[c]:
            copy.wait_recv()
        taken = jnp.concatenate([s.pair[b, c].reshape(run, model) for b in range(2)], axis=0)
        normed = norm_rows(taken, s.eg[...])
        values = [dot_nt(normed, matrix(m)).astype(BF) for m in range(3)]
        values[0] = values[0] * BF(HDIM ** (-0.5))
        for b in range(2):
            at = b * BLK + c * run
            s.q[at : at + run] = values[0][b * run : (b + 1) * run]
            s.k[at : at + run] = values[1][b * run : (b + 1) * run]
            for slab in range(model // LANES):
                s.v[at : at + run, 2 * slab * LANES : (2 * slab + 1) * LANES] = values[2][
                    b * run : (b + 1) * run, slab * LANES : (slab + 1) * LANES
                ]

    def forward(m):
        to_peer[m].wait_recv()
        passed[m].start()

    for c in range(STEPS):
        swap(c)
        if c == STEPS - 2:
            for m in range(4):
                forward(m)
            for m in range(3):
                to_partner[m].wait_recv()
                passed[m].wait_recv()
            for early in range(c):
                project(early)
    project(STEPS - 2)
    project(STEPS - 1)
    to_partner[3].wait_recv()
    passed[3].wait_recv()

    apart = jnp.where(same > 0, 0.0, -1e30).astype(F32)
    key_block = lax.broadcasted_iota(jnp.int32, (1, PAIR), 1) // BLK
    first = lax.broadcasted_iota(jnp.int32, (CHUNK, LANES), 1) < HDIM
    chunks = PAIR // CHUNK

    def emb_copies(i):
        at = pl.ds(pl.multiple_of(i * CHUNK, CHUNK), CHUNK)
        mine, theirs = s.emb.at[head, at], s.emb.at[peer, at]
        return types.SimpleNamespace(
            peer=remote(mine, mine, s.gs.at[0, i], s.gr.at[0, i], (seq, peer)),
            partner=remote(mine, mine, s.gs.at[1, i], s.gr.at[1, i], (seq, partner)),
            across=remote(theirs, theirs, s.gs.at[2, i], s.gr.at[2, i], (seq, partner)),
        )

    per_chunk = CHUNK // run

    def attend(i):
        at = pl.ds(pl.multiple_of(i * CHUNK, CHUNK), CHUNK)
        block = lax.div(i, BLK // CHUNK)
        bias = jnp.where(key_block == block, 0.0, apart)
        for slab in range(model // LANES):
            columns = slice(slab * LANES, (slab + 1) * LANES)
            query = s.q[at, columns]
            nothing = jnp.zeros_like(query)
            both = jnp.concatenate(
                [jnp.where(first, query, nothing), jnp.where(first, nothing, query)], axis=0
            )
            scores = dot_nt(both, s.k[:, columns]) + bias
            top = jnp.max(scores, axis=-1, keepdims=True)
            weights = jnp.exp(scores - top).astype(BF)
            mixed = dot(weights, s.v[:, 2 * slab * LANES : 2 * (slab + 1) * LANES])
            mixed = mixed[:, :LANES] * (1.0 / mixed[:, LANES:])
            s.a[:, columns] = jnp.where(first, mixed[:CHUNK], mixed[CHUNK:]).astype(BF)
        mixed = dot(s.a[...], matrix(3))
        low = lax.rem(i, BLK // CHUNK) * per_chunk
        taken = s.pair[block, pl.ds(low, per_chunk)].reshape(CHUNK, model)
        s.emb[head, at] = (taken.astype(F32) + mixed).astype(BF)

    scale = RATE_SCALE * (tokens * n) ** (-0.5)

    def fast_project(owner, i):
        at = pl.ds(pl.multiple_of(owner * PAIR + i * CHUNK, CHUNK), CHUNK)
        normed = norm_rows(s.emb[owner, pl.ds(i * CHUNK, CHUNK)], s.fg[...])
        mapped = dot_nt(normed, s.wf[...])
        s.fq[at] = mapped[:, :wide].astype(BF)
        key = mapped[:, wide : 2 * wide].astype(BF)
        s.fkt[:, at] = key.T
        value = mapped[:, 2 * wide :].astype(BF).astype(F32)
        before = mapped[:, rate_at : rate_at + 1]
        soft = jnp.maximum(before, 0.0) + jnp.log1p(jnp.exp(-jnp.abs(before)))
        back = (-(scale * soft) * value).astype(BF)
        s.ogt[:, at] = back.T
        for part in range(parts):
            both = dot(key, s.guw[part])
            gate, up = both[:, :LANES], both[:, LANES:]
            grad = dot(back, s.dth[:, part * LANES : (part + 1) * LANES])
            sig = jax.nn.sigmoid(gate)
            silu = gate * sig
            s.hk[part, at] = (silu * up).astype(BF)
            s.two[part, at, :LANES] = (grad * up * sig * (1.0 + gate * (1.0 - sig))).astype(BF)
            s.two[part, at, LANES:] = (grad * silu).astype(BF)

    across = lax.rem(partner + nh // 2, nh)

    def take_partner(i):
        emb_copies(i).partner.wait_recv()

    def take_peer(i):
        copies = emb_copies(i)
        copies.peer.wait_recv()
        copies.across.start()

    def own_chunk(i, carry):
        attend(i)
        copies = emb_copies(i)
        copies.peer.start()
        copies.partner.start()

        def one(which, inside):
            at = i - which

            @pl.when(at >= 0)
            def _():
                @pl.when(which == 1)
                def _():
                    take_partner(at)

                @pl.when(which == 2)
                def _():
                    take_peer(at)

                owner = jnp.where(which == 0, head, jnp.where(which == 1, partner, peer))
                fast_project(owner, at)

            return inside

        return lax.fori_loop(0, 3, one, carry)

    lax.fori_loop(0, chunks, own_chunk, 0)
    take_partner(chunks - 1)
    fast_project(partner, chunks - 1)
    emb_copies(0).across.wait_recv()
    fast_project(across, 0)
    take_peer(chunks - 2)
    fast_project(peer, chunks - 2)
    for i in range(1, chunks - 1):
        emb_copies(i).across.wait_recv()
        fast_project(across, i)
    take_peer(chunks - 1)
    fast_project(peer, chunks - 1)
    emb_copies(chunks - 1).across.wait_recv()
    fast_project(across, chunks - 1)

    def compute(part):
        one = dot(s.fkt[...], s.two[part])
        other = dot(s.ogt[...], s.hk[part])
        s.g[0:width] = one[:width, :LANES]
        s.g[width : 2 * width] = one[:width, LANES:]
        s.g[2 * width : 3 * width] = other[:width]
        chunk = s.part.shape[3]
        for i in range(2):
            for o in range(outer_count):
                at = (i * outer_count + o) * chunk
                s.part[part, i, o] = s.g[at : at + chunk].astype(BF)

    def during():
        for which in range(model // width):

            @pl.when(head == which)
            def _():
                for owner in range(nh):
                    at = owner * PAIR
                    s.col[at : at + PAIR] = s.emb[owner, :, which * width : (which + 1) * width]

    gradient_sum(n, width, s, side, lane, compute, during)

    for which in range(2):
        start = s.gu[which]
        fresh = renorm(start - s.total[which * width : (which + 1) * width], start, 1)
        s.ag[:width, which * hidden : (which + 1) * hidden] = fresh.astype(BF)
    start = s.dt[...]
    s.ad[...] = renorm(start - s.total[2 * width : 3 * width], start, 0).astype(BF)

    def put(unit):
        at = pl.ds(unit * BLK, BLK)
        return pltpu.make_async_copy(s.done.at[at], o_ref.at[at], s.put.at[unit])

    def final(unit, carry):
        base = pl.multiple_of(unit * BLK, BLK)
        at = pl.ds(base, BLK)
        both = dot(s.fq[at], s.ag[...])
        gate = both[:, :hidden]
        inside = (gate * jax.nn.sigmoid(gate) * both[:, hidden:]).astype(BF)
        done = (s.col[at].astype(F32) + dot_nt(inside, s.ad[...])).astype(BF)
        for c in range(STEPS):
            for which in range(per_block):
                low = (c * per_block + which) * rows
                to = pl.multiple_of(base + which * STEPS * rows + c * rows, rows)
                s.done[pl.ds(to, rows)] = done[low : low + rows]
        put(unit).start()
        return carry

    lax.fori_loop(0, tokens // BLK, final, 0, unroll=2)
    for unit in range(tokens // BLK):
        put(unit).wait()

    for copy in meta_copies + to_peer + to_partner + passed:
        copy.wait_send()
    for group in x_copies + swaps:
        for copy in group:
            copy.wait_send()
    for i in range(chunks):
        copies = emb_copies(i)
        for copy in (copies.peer, copies.partner, copies.across):
            copy.wait_send()


def on_device(
    patches,
    slot_image,
    slot_dest,
    enc_gain,
    w_qkv,
    w_out,
    fast_gain,
    w_fast,
    w_rate,
    fast_gate_up,
    fast_down,
):
    n = lax.axis_size("seq")
    nh = lax.axis_size("head")
    model = patches.shape[1]
    slots = slot_dest.shape[0]
    width, hidden = fast_gate_up.shape[2:]
    part = PAIR // nh
    sizes = layout(n, nh, slots, model, width, hidden)
    return pl.pallas_call(
        functools.partial(whole_kernel, n, nh, tuple(sizes)),
        out_shape=jax.ShapeDtypeStruct((nh * PAIR, width), patches.dtype),
        in_specs=[SMEM, SMEM] + [ANY] * 9,
        out_specs=ANY,
        scratch_shapes=list(sizes.values()),
        compiler_params=pltpu.CompilerParams(
            collective_id=1, has_side_effects=True, vmem_limit_bytes=60 * 1024 * 1024
        ),
        name="encode_and_update",
    )(
        slot_dest,
        slot_image,
        patches.reshape(slots, BLK // part, STEPS, part // STEPS, model),
        jnp.swapaxes(w_qkv, 1, 2),
        w_out,
        enc_gain.reshape(model // LANES, LANES),
        fast_gain.reshape(model // LANES, LANES),
        jnp.swapaxes(w_fast, 1, 2),
        w_rate.T,
        fast_gate_up[0],
        fast_down[0].T,
    )


def solution(mesh):
    in_specs = (
        P("seq", None),
        P("seq"),
        P("seq"),
        P(),
        P(None, None, "head"),
        P("head", None),
        P(),
        P(None, None, "head"),
        P(None, "head"),
        P("head", None, None, None),
        P("head", None, None),
    )
    out_specs = P("seq", "head")
    return jax.shard_map(
        on_device, mesh=mesh, in_specs=in_specs, out_specs=out_specs, check_vma=False
    )
```

```python
import functools
import types

import jax
import jax.numpy as jnp
from jax import lax
from jax.experimental import pallas as pl
from jax.experimental.pallas import tpu as pltpu
from jax.sharding import PartitionSpec as P

HDIM = 64
BLK = 256
BLK_DEV = 8
PAIR = 2 * BLK
EPSILON = 1e-06
RATE_SCALE = 0.1
LANES = 128
STEPS = 8
CHUNK = 128
UNIT = 256
MESH = pl.DeviceIdType.MESH
VMEM = pl.BlockSpec(memory_space=pltpu.VMEM)
SMEM = pl.BlockSpec(memory_space=pltpu.SMEM)
ANY = pl.BlockSpec(memory_space=pl.ANY)
NT = (((1,), (1,)), ((), ()))
BF = jnp.bfloat16
F32 = jnp.float32


def remote(src, dst, send, recv, device):
    return pltpu.make_async_remote_copy(
        src_ref=src, dst_ref=dst, send_sem=send, recv_sem=recv, device_id=device, device_id_type=MESH
    )


def others(axis_size, me):
    return [lax.rem(me + step, axis_size) for step in range(1, axis_size)]


def dot(a, b):
    return jnp.dot(a, b, preferred_element_type=F32)


def dot_nt(a, b):
    return lax.dot_general(a, b, NT, preferred_element_type=F32)


def norm_rows(values, gain):
    wide = values.astype(F32)
    factor = lax.rsqrt(jnp.mean(wide * wide, axis=-1, keepdims=True) + EPSILON)
    return (wide * factor * gain).astype(BF)


def renorm(updated, initial, axis):
    target_norm = jnp.sqrt(jnp.sum(initial * initial, axis=axis, keepdims=True))
    return (
        updated
        * target_norm
        * lax.rsqrt(jnp.sum(updated * updated, axis=axis, keepdims=True) + EPSILON)
    )


def layout(n, nh, slots, model, width, hidden):
    vmem, dma = pltpu.VMEM, pltpu.SemaphoreType.DMA
    part = PAIR // nh
    rows = part // STEPS
    wide = LANES * (-(-width // LANES))
    tokens = nh * PAIR
    parts = hidden // LANES
    chunk = 8 * (-(-3 * width // (8 * n)))
    outer = n // 2
    sizes = {}
    for c in range(STEPS):
        sizes[f"held{c}"] = vmem((slots, rows, model), BF)
        sizes[f"out{c}"] = vmem((n, rows, model), BF)
        sizes[f"in{c}"] = vmem((n, rows, model), BF)
        sizes[f"chosen{c}"] = vmem((nh, rows, model), BF)
    sizes.update(
        meta=vmem((n, 1, LANES), jnp.int32), meta_in=vmem((n, 1, LANES), jnp.int32),
        codes=pltpu.SMEM((n, 1, LANES), jnp.int32),
        w=vmem((4, nh, width, model), BF),
        pair=vmem((2, STEPS, nh // 2, rows, model), BF),
        q=vmem((PAIR, model), BF), k=vmem((PAIR, model), BF), v=vmem((PAIR, 2 * model), BF),
        a=vmem((CHUNK, model), BF), emb=vmem((nh, PAIR, model), BF),
        wf_in=vmem((3, width, model), BF), wr_in=vmem((1, model), BF),
        gu=vmem((2, width, hidden), F32), dt=vmem((width, hidden), F32),
        wf=vmem((3 * wide, model), BF), fq=vmem((tokens, wide), BF),
        fkt=vmem((wide, tokens), BF), ogt=vmem((wide, tokens), BF),
        col=vmem((tokens, width), BF), two=vmem((parts, tokens, 2 * LANES), BF),
        hk=vmem((parts, tokens, LANES), BF),
        guw=vmem((parts, wide, 2 * LANES), BF), dth=vmem((wide, hidden), BF),
        g=vmem((max(3 * width, chunk * n), LANES), F32),
        total=vmem((max(3 * width, chunk * n), hidden), F32),
        ag=vmem((wide, 2 * hidden), BF), ad=vmem((width, hidden), BF),
        part=vmem((parts, 2, outer, chunk, LANES), BF), xin=vmem((parts, outer, chunk, LANES), BF),
        half=vmem((parts, outer, chunk, LANES), BF), zin=vmem((parts, outer - 1, chunk, LANES), BF),
        res=vmem((parts, 2, outer, chunk, LANES), BF),
        eg_in=vmem((model // LANES, LANES), F32), fg_in=vmem((model // LANES, LANES), F32),
        eg=vmem((1, model), F32), fg=vmem((1, model), F32), done=vmem((tokens, width), BF),
        local=dma((STEPS + 9,)), put=dma((tokens // BLK,)),
        xs=dma((STEPS, n - 1)), xr=dma((STEPS, n - 1)), ms=dma((n - 1,)), mr=dma((n - 1,)),
        ws=dma((3, 4)), wr=dma((3, 4)), ss=dma((STEPS, nh - 1)), sr=dma((STEPS, nh - 1)),
        gs=dma((3, PAIR // CHUNK)), gr=dma((3, PAIR // CHUNK)),
        ps=dma((parts,)), pr=dma((parts,)), zs=dma((parts, outer - 1)), zr=dma((parts, outer - 1)),
        rs=dma((parts, outer)), rr=dma((parts, outer)),
        fs=dma((parts, outer - 1)), fr=dma((parts, outer - 1)),
    )
    return sizes


def gradient_sum(n, width, s, side, lane, compute, during):
    seq = lax.axis_index("seq")
    outer_count = n // 2
    inner, outer = lax.rem(seq, 2), lax.div(seq, 2)
    parts = s.part.shape[0]
    chunk = s.part.shape[3]
    steps = range(1, outer_count)

    def plan(part):
        mine = s.res.at[part, inner, outer]
        theirs = [s.res.at[part, inner, lax.rem(outer + outer_count - t, outer_count)] for t in steps]
        return types.SimpleNamespace(
            x=remote(s.part.at[part, 1 - inner], s.xin.at[part], s.ps.at[part], s.pr.at[part], side),
            z=[
                remote(
                    s.half.at[part, lax.rem(outer + t, outer_count)], s.zin.at[part, t - 1],
                    s.zs.at[part, t - 1], s.zr.at[part, t - 1], lane[t - 1],
                )
                for t in steps
            ],
            r=[
                remote(mine, mine, s.rs.at[part, t], s.rr.at[part, t], to)
                for t, to in enumerate(lane + [side])
            ],
            f=[
                remote(theirs[t - 1], theirs[t - 1], s.fs.at[part, t - 1], s.fr.at[part, t - 1], side)
                for t in steps
            ],
        )

    plans = [plan(part) for part in range(parts)]

    def stage_x(part):
        plans[part].x.start()

    def stage_z(part):
        plans[part].x.wait_recv()
        for o in range(outer_count):
            s.half[part, o] = (
                s.part[part, inner, o].astype(F32) + s.xin[part, o].astype(F32)
            ).astype(BF)
        for copy in plans[part].z:
            copy.start()

    def stage_r(part):
        total = s.half[part, outer].astype(F32)
        for t, copy in enumerate(plans[part].z):
            copy.wait_recv()
            total = total + s.zin[part, t].astype(F32)
        s.res[part, inner, outer] = total.astype(BF)
        for copy in plans[part].r:
            copy.start()

    def stage_f(part):
        for t in steps:
            plans[part].r[t - 1].wait_recv()
            plans[part].f[t - 1].start()

    for part in range(parts):
        compute(part)
        stage_x(part)
    for part in range(parts):
        stage_z(part)
    during()
    for part in range(parts):
        stage_r(part)
    for part in range(parts):
        stage_f(part)
    for part in range(parts):
        plans[part].r[-1].wait_recv()
        for copy in plans[part].f:
            copy.wait_recv()
        cut = slice(part * LANES, (part + 1) * LANES)
        for i in range(2):
            for o in range(outer_count):
                at = (i * outer_count + o) * chunk
                s.total[at : at + chunk, cut] = s.res[part, i, o].astype(F32)
    for part in range(parts):
        plans[part].x.wait_send()
        for copy in plans[part].z + plans[part].r + plans[part].f:
            copy.wait_send()


def whole_kernel(
    n, nh, names, dest_ref, image_ref, x_ref, wqkv_ref, wo_ref, eg_ref, fg_ref, wf_ref, wr_ref,
    gu_ref, dt_ref, o_ref, *scratch,
):
    s = types.SimpleNamespace(**dict(zip(names, scratch)))
    seq, head = lax.axis_index("seq"), lax.axis_index("head")
    partner = head + 1 - 2 * lax.rem(head, 2)
    peer = lax.rem(head + nh // 2, nh)
    targets = others(n, seq)
    mates = others(nh, head)
    outer_count = n // 2
    inner, outer = lax.rem(seq, 2), lax.div(seq, 2)
    side = (outer * 2 + 1 - inner, head)
    lane = [(lax.rem(outer + t, outer_count) * 2 + inner, head) for t in range(1, outer_count)]
    model = x_ref.shape[-1]
    width, hidden = gu_ref.shape[1:]
    wide = s.fq.shape[1]
    parts = hidden // LANES
    tokens = nh * PAIR
    held = [getattr(s, f"held{c}") for c in range(STEPS)]
    out = [getattr(s, f"out{c}") for c in range(STEPS)]
    arrived = [getattr(s, f"in{c}") for c in range(STEPS)]
    chosen = [getattr(s, f"chosen{c}") for c in range(STEPS)]
    rows = held[0].shape[1]
    per_block = nh // 2

    barrier = pltpu.get_barrier_semaphore()
    greeted = [(to, head) for to in targets] + [(seq, to) for to in mates]
    for device in greeted:
        pl.semaphore_signal(barrier, inc=1, device_id=device, device_id_type=MESH)

    fetch = [
        pltpu.make_async_copy(x_ref.at[:, lax.rem(head, per_block), c], held[c], s.local.at[c])
        for c in range(STEPS)
    ]
    weights_in = [
        pltpu.make_async_copy(wqkv_ref, s.w.at[0:3, head], s.local.at[STEPS]),
        pltpu.make_async_copy(wo_ref, s.w.at[3, head], s.local.at[STEPS + 1]),
    ]
    late = [
        pltpu.make_async_copy(src, dst, s.local.at[STEPS + 2 + which])
        for which, (src, dst) in enumerate(
            [(wf_ref, s.wf_in), (wr_ref, s.wr_in), (gu_ref, s.gu), (dt_ref, s.dt)]
        )
    ]
    gains_in = [
        pltpu.make_async_copy(src, dst, s.local.at[STEPS + 7 + which])
        for which, (src, dst) in enumerate([(eg_ref, s.eg_in), (fg_ref, s.fg_in)])
    ]
    for copy in fetch[:1] + weights_in + fetch[1:] + late + gains_in:
        copy.start()

    my_block = lax.div(head, per_block)
    pairs = dest_ref.shape[0] // 2
    firsts = [dest_ref[2 * i] for i in range(pairs)]
    sames = [(image_ref[2 * i] == image_ref[2 * i + 1]).astype(jnp.int32) for i in range(pairs)]
    homes = [lax.div(jnp.maximum(d, 0), BLK_DEV) for d in firsts]
    slots = []
    for i, d in enumerate(firsts):
        slots.append(2 * i + lax.rem(jnp.maximum(d, 0) + my_block, 2))
    marks = [
        2 * lax.div(lax.rem(jnp.maximum(d, 0), BLK_DEV), 2) + same for d, same in zip(firsts, sames)
    ]

    def lookup(target):
        slot, code = jnp.int32(0), jnp.int32(-1)
        for i, d in enumerate(firsts):
            hit = jnp.logical_and(d >= 0, homes[i] == target)
            slot = jnp.where(hit, slots[i], slot)
            code = jnp.where(hit, marks[i], code)
        return slot, code

    found = [lookup(to) for to in targets + [seq]]
    for step, to in enumerate(targets):
        s.meta[step] = jnp.full((1, LANES), found[step][1], jnp.int32)
    s.meta_in[seq] = jnp.full((1, LANES), found[-1][1], jnp.int32)

    def pick(c):
        fetch[c].wait()
        for step in range(n - 1):
            out[c][step] = held[c][found[step][0]]
        arrived[c][seq] = held[c][found[-1][0]]

    meta_copies = [
        remote(s.meta.at[step], s.meta_in.at[seq], s.ms.at[step], s.mr.at[step], (to, head))
        for step, to in enumerate(targets)
    ]
    x_copies = [
        [
            remote(out[c].at[step], arrived[c].at[seq], s.xs.at[c, step], s.xr.at[c, step], (to, head))
            for step, to in enumerate(targets)
        ]
        for c in range(STEPS)
    ]
    to_peer = [
        remote(s.w.at[m, head], s.w.at[m, head], s.ws.at[0, m], s.wr.at[0, m], (seq, peer))
        for m in range(4)
    ]
    to_partner = [
        remote(s.w.at[m, head], s.w.at[m, head], s.ws.at[1, m], s.wr.at[1, m], (seq, partner))
        for m in range(4)
    ]
    passed = [
        remote(s.w.at[m, peer], s.w.at[m, peer], s.ws.at[2, m], s.wr.at[2, m], (seq, partner))
        for m in range(4)
    ]
    pick(0)
    pl.semaphore_wait(barrier, len(greeted))
    far_first = sorted(range(n - 1), key=lambda step: abs(step + 1 - n // 2))
    for copy in meta_copies + [x_copies[0][step] for step in far_first]:
        copy.start()
    for copy in weights_in:
        copy.wait()
    for copy in to_peer + to_partner:
        copy.start()
    for c in range(1, STEPS):
        pick(c)
        for step in far_first:
            x_copies[c][step].start()

    s.wf[...] = jnp.zeros_like(s.wf)
    s.v[...] = jnp.ones_like(s.v)
    s.guw[...] = jnp.zeros_like(s.guw)
    s.dth[...] = jnp.zeros_like(s.dth)
    s.g[...] = jnp.zeros_like(s.g)
    s.ag[...] = jnp.zeros_like(s.ag)
    for copy in late + gains_in:
        copy.wait()
    for src, dst in ((s.eg_in, s.eg), (s.fg_in, s.fg)):
        for which in range(model // LANES):
            dst[:, which * LANES : (which + 1) * LANES] = src[which : which + 1]
    for which in range(3):
        s.wf[which * wide : which * wide + width] = s.wf_in[which]
    rate_at = 2 * wide + width
    s.wf[rate_at : rate_at + 16] = jnp.broadcast_to(s.wr_in[...], (16, model))
    s.dth[:width] = s.dt[...].astype(BF)
    for part in range(parts):
        cut = slice(part * LANES, (part + 1) * LANES)
        s.guw[part, :width, :LANES] = s.gu[0, :, cut].astype(BF)
        s.guw[part, :width, LANES:] = s.gu[1, :, cut].astype(BF)

    for copy in meta_copies:
        copy.wait_recv()
    spread = pltpu.make_async_copy(s.meta_in, s.codes, s.local.at[STEPS + 6])
    spread.start()
    spread.wait()
    sources = [jnp.int32(0)] * nh
    same = jnp.int32(0)
    for source in range(n):
        code = s.codes[source, 0, 0]
        place = lax.div(jnp.maximum(code, 0), 2)
        for p in range(nh):
            sources[p] = jnp.where(jnp.logical_and(code >= 0, place == p), source, sources[p])
        mine = jnp.logical_and(code >= 0, place == head)
        same = jnp.where(mine, lax.rem(jnp.maximum(code, 0), 2), same)

    swaps = [
        [
            remote(
                chosen[c].at[to], s.pair.at[lax.div(head, per_block), c, lax.rem(head, per_block)],
                s.ss.at[c, step], s.sr.at[c, step], (seq, to),
            )
            for step, to in enumerate(mates)
        ]
        for c in range(STEPS)
    ]

    def swap(c):
        for copy in x_copies[c]:
            copy.wait_recv()
        for p in range(nh):
            chosen[c][p] = arrived[c][sources[p]]
        for copy in swaps[c]:
            copy.start()
        s.pair[lax.div(head, per_block), c, lax.rem(head, per_block)] = chosen[c][head]

    def matrix(m):
        return s.w[m].reshape(nh * width, model)

    run = per_block * rows

    def project(c):
        for copy in swaps[c]:
            copy.wait_recv()
        taken = jnp.concatenate([s.pair[b, c].reshape(run, model) for b in range(2)], axis=0)
        normed = norm_rows(taken, s.eg[...])
        values = [dot_nt(normed, matrix(m)).astype(BF) for m in range(3)]
        values[0] = values[0] * BF(HDIM ** (-0.5))
        for b in range(2):
            at = b * BLK + c * run
            s.q[at : at + run] = values[0][b * run : (b + 1) * run]
            s.k[at : at + run] = values[1][b * run : (b + 1) * run]
            for slab in range(model // LANES):
                s.v[at : at + run, 2 * slab * LANES : (2 * slab + 1) * LANES] = values[2][
                    b * run : (b + 1) * run, slab * LANES : (slab + 1) * LANES
                ]

    def forward(m):
        to_peer[m].wait_recv()
        passed[m].start()

    for c in range(STEPS):
        swap(c)
        if c == STEPS - 2:
            for m in range(4):
                forward(m)
            for m in range(3):
                to_partner[m].wait_recv()
                passed[m].wait_recv()
            for early in range(c):
                project(early)
    project(STEPS - 2)
    project(STEPS - 1)
    to_partner[3].wait_recv()
    passed[3].wait_recv()

    apart = jnp.where(same > 0, 0.0, -1e30).astype(F32)
    key_block = lax.broadcasted_iota(jnp.int32, (1, PAIR), 1) // BLK
    first = lax.broadcasted_iota(jnp.int32, (CHUNK, LANES), 1) < HDIM
    chunks = PAIR // CHUNK

    def emb_copies(i):
        at = pl.ds(pl.multiple_of(i * CHUNK, CHUNK), CHUNK)
        mine, theirs = s.emb.at[head, at], s.emb.at[peer, at]
        return types.SimpleNamespace(
            peer=remote(mine, mine, s.gs.at[0, i], s.gr.at[0, i], (seq, peer)),
            partner=remote(mine, mine, s.gs.at[1, i], s.gr.at[1, i], (seq, partner)),
            across=remote(theirs, theirs, s.gs.at[2, i], s.gr.at[2, i], (seq, partner)),
        )

    per_chunk = CHUNK // run

    def attend(i):
        at = pl.ds(pl.multiple_of(i * CHUNK, CHUNK), CHUNK)
        block = lax.div(i, BLK // CHUNK)
        bias = jnp.where(key_block == block, 0.0, apart)
        for slab in range(model // LANES):
            columns = slice(slab * LANES, (slab + 1) * LANES)
            query = s.q[at, columns]
            nothing = jnp.zeros_like(query)
            both = jnp.concatenate(
                [jnp.where(first, query, nothing), jnp.where(first, nothing, query)], axis=0
            )
            scores = dot_nt(both, s.k[:, columns]) + bias
            top = jnp.max(scores, axis=-1, keepdims=True)
            weights = jnp.exp(scores - top).astype(BF)
            mixed = dot(weights, s.v[:, 2 * slab * LANES : 2 * (slab + 1) * LANES])
            mixed = mixed[:, :LANES] * (1.0 / mixed[:, LANES:])
            s.a[:, columns] = jnp.where(first, mixed[:CHUNK], mixed[CHUNK:]).astype(BF)
        mixed = dot(s.a[...], matrix(3))
        low = lax.rem(i, BLK // CHUNK) * per_chunk
        taken = s.pair[block, pl.ds(low, per_chunk)].reshape(CHUNK, model)
        s.emb[head, at] = (taken.astype(F32) + mixed).astype(BF)

    scale = RATE_SCALE * (tokens * n) ** (-0.5)

    def fast_project(owner, i):
        at = pl.ds(pl.multiple_of(owner * PAIR + i * CHUNK, CHUNK), CHUNK)
        normed = norm_rows(s.emb[owner, pl.ds(i * CHUNK, CHUNK)], s.fg[...])
        mapped = dot_nt(normed, s.wf[...])
        s.fq[at] = mapped[:, :wide].astype(BF)
        key = mapped[:, wide : 2 * wide].astype(BF)
        s.fkt[:, at] = key.T
        value = mapped[:, 2 * wide :].astype(BF).astype(F32)
        before = mapped[:, rate_at : rate_at + 1]
        soft = jnp.maximum(before, 0.0) + jnp.log1p(jnp.exp(-jnp.abs(before)))
        back = (-(scale * soft) * value).astype(BF)
        s.ogt[:, at] = back.T
        for part in range(parts):
            both = dot(key, s.guw[part])
            gate, up = both[:, :LANES], both[:, LANES:]
            grad = dot(back, s.dth[:, part * LANES : (part + 1) * LANES])
            sig = jax.nn.sigmoid(gate)
            silu = gate * sig
            s.hk[part, at] = (silu * up).astype(BF)
            s.two[part, at, :LANES] = (grad * up * sig * (1.0 + gate * (1.0 - sig))).astype(BF)
            s.two[part, at, LANES:] = (grad * silu).astype(BF)

    across = lax.rem(partner + nh // 2, nh)

    def take_partner(i):
        emb_copies(i).partner.wait_recv()

    def take_peer(i):
        copies = emb_copies(i)
        copies.peer.wait_recv()
        copies.across.start()

    def own_chunk(i, carry):
        attend(i)
        copies = emb_copies(i)
        copies.peer.start()
        copies.partner.start()

        def one(which, inside):
            at = i - which

            @pl.when(at >= 0)
            def _():
                @pl.when(which == 1)
                def _():
                    take_partner(at)

                @pl.when(which == 2)
                def _():
                    take_peer(at)

                owner = jnp.where(which == 0, head, jnp.where(which == 1, partner, peer))
                fast_project(owner, at)

            return inside

        return lax.fori_loop(0, 3, one, carry)

    lax.fori_loop(0, chunks, own_chunk, 0)
    take_partner(chunks - 1)
    fast_project(partner, chunks - 1)
    emb_copies(0).across.wait_recv()
    fast_project(across, 0)
    take_peer(chunks - 2)
    fast_project(peer, chunks - 2)
    for i in range(1, chunks - 1):
        emb_copies(i).across.wait_recv()
        fast_project(across, i)
    take_peer(chunks - 1)
    fast_project(peer, chunks - 1)
    emb_copies(chunks - 1).across.wait_recv()
    fast_project(across, chunks - 1)

    def compute(part):
        one = dot(s.fkt[...], s.two[part])
        other = dot(s.ogt[...], s.hk[part])
        s.g[0:width] = one[:width, :LANES]
        s.g[width : 2 * width] = one[:width, LANES:]
        s.g[2 * width : 3 * width] = other[:width]
        chunk = s.part.shape[3]
        for i in range(2):
            for o in range(outer_count):
                at = (i * outer_count + o) * chunk
                s.part[part, i, o] = s.g[at : at + chunk].astype(BF)

    def during():
        for which in range(model // width):

            @pl.when(head == which)
            def _():
                for owner in range(nh):
                    at = owner * PAIR
                    s.col[at : at + PAIR] = s.emb[owner, :, which * width : (which + 1) * width]

    gradient_sum(n, width, s, side, lane, compute, during)

    for which in range(2):
        start = s.gu[which]
        fresh = renorm(start - s.total[which * width : (which + 1) * width], start, 1)
        s.ag[:width, which * hidden : (which + 1) * hidden] = fresh.astype(BF)
    start = s.dt[...]
    s.ad[...] = renorm(start - s.total[2 * width : 3 * width], start, 0).astype(BF)

    def put(unit):
        at = pl.ds(unit * BLK, BLK)
        return pltpu.make_async_copy(s.done.at[at], o_ref.at[at], s.put.at[unit])

    def final(unit, carry):
        base = pl.multiple_of(unit * BLK, BLK)
        at = pl.ds(base, BLK)
        both = dot(s.fq[at], s.ag[...])
        gate = both[:, :hidden]
        inside = (gate * jax.nn.sigmoid(gate) * both[:, hidden:]).astype(BF)
        done = (s.col[at].astype(F32) + dot_nt(inside, s.ad[...])).astype(BF)
        for c in range(STEPS):
            for which in range(per_block):
                low = (c * per_block + which) * rows
                to = pl.multiple_of(base + which * STEPS * rows + c * rows, rows)
                s.done[pl.ds(to, rows)] = done[low : low + rows]
        put(unit).start()
        return carry

    lax.fori_loop(0, tokens // BLK, final, 0, unroll=2)
    for unit in range(tokens // BLK):
        put(unit).wait()

    for copy in meta_copies + to_peer + to_partner + passed:
        copy.wait_send()
    for group in x_copies + swaps:
        for copy in group:
            copy.wait_send()
    for i in range(chunks):
        copies = emb_copies(i)
        for copy in (copies.peer, copies.partner, copies.across):
            copy.wait_send()


def on_device(
    patches,
    slot_image,
    slot_dest,
    enc_gain,
    w_qkv,
    w_out,
    fast_gain,
    w_fast,
    w_rate,
    fast_gate_up,
    fast_down,
):
    n = lax.axis_size("seq")
    nh = lax.axis_size("head")
    model = patches.shape[1]
    slots = slot_dest.shape[0]
    width, hidden = fast_gate_up.shape[2:]
    part = PAIR // nh
    sizes = layout(n, nh, slots, model, width, hidden)
    return pl.pallas_call(
        functools.partial(whole_kernel, n, nh, tuple(sizes)),
        out_shape=jax.ShapeDtypeStruct((nh * PAIR, width), patches.dtype),
        in_specs=[SMEM, SMEM] + [ANY] * 9,
        out_specs=ANY,
        scratch_shapes=list(sizes.values()),
        compiler_params=pltpu.CompilerParams(
            collective_id=1, has_side_effects=True, vmem_limit_bytes=60 * 1024 * 1024
        ),
        name="encode_and_update",
    )(
        slot_dest,
        slot_image,
        patches.reshape(slots, BLK // part, STEPS, part // STEPS, model),
        jnp.swapaxes(w_qkv, 1, 2),
        w_out,
        enc_gain.reshape(model // LANES, LANES),
        fast_gain.reshape(model // LANES, LANES),
        jnp.swapaxes(w_fast, 1, 2),
        w_rate.T,
        fast_gate_up[0],
        fast_down[0].T,
    )


def solution(mesh):
    in_specs = (
        P("seq", None),
        P("seq"),
        P("seq"),
        P(),
        P(None, None, "head"),
        P("head", None),
        P(),
        P(None, None, "head"),
        P(None, "head"),
        P("head", None, None, None),
        P("head", None, None),
    )
    out_specs = P("seq", "head")
    return jax.shard_map(
        on_device, mesh=mesh, in_specs=in_specs, out_specs=out_specs, check_vma=False
    )
```
